8 devices in a mesh: rep: 1 (over z), data: 2 (over y), expert: 4 (over x, core).
Axes of the slice: x: 2, y: 2, z: 1, core: 2. Of those that a mesh axis runs over, the one named last changes fastest.
Arguments:
- x: bfloat16 [128, 128, 2304], P(('rep', 'expert', 'data'))
- expert_idx: int32 [128, 128, 2], P(('rep', 'expert', 'data'))
- gate: float32 [128, 128, 2], P(('rep', 'expert', 'data'))
- attn_gain: float32 [2304], replicated
- w_qkv: bfloat16 [2304, 108, 64], P(('data', 'expert'))
- w_out: bfloat16 [36, 64, 2304], P(None, None, ('data', 'expert'))
- moe_gain: float32 [2304], replicated
- w_gate: bfloat16 [8, 2304, 5760], P('expert', 'data')
- w_up: bfloat16 [8, 2304, 5760], P('expert', 'data')
- w_down: bfloat16 [8, 5760, 2304], P('expert', None, 'data')
Outputs:
- output: bfloat16 [128, 128, 2304], P(('rep', 'expert', 'data'))
All inputs are finite; a program needn't handle non-finite values.
Results may differ from the reference program's by a relative error of at most 0.0147271.
Values are sent between devices in bfloat16 or wider.
A program may use at most 1 GiB of HBM per device.

```python
import jax
import jax.numpy as jnp
from jax import lax

MODEL_DIM = 2304
EXPERT_FF = 5760
EXPERTS = 8
TOP_K = 2
NUM_HEADS = 36
KV_HEADS = 36
HEAD_DIM = 64
SEQ_LEN = 128
SEQS_DEV = 16
EXPERT_AXIS = 4
DATA_AXIS = 2

TOK_DEV = SEQS_DEV * SEQ_LEN
GROUP_DEVS = EXPERT_AXIS * DATA_AXIS
CAPACITY = 8 * ((5 * TOP_K * TOK_DEV + 32 * EXPERTS - 1) // (32 * EXPERTS))
QKV_HEADS = NUM_HEADS + 2 * KV_HEADS
GROUP_LEN = NUM_HEADS // KV_HEADS
NORM_EPS = 1e-6
ROPE_BASE = 10000.0


def draw_routing(key):
    noise_key, hot_key, perm_key = jax.random.split(key, 3)
    noise = jax.random.randint(noise_key, (GROUP_DEVS, TOK_DEV, EXPERTS), 0, 1 << 20)
    hot_ids = jax.random.randint(hot_key, (GROUP_DEVS,), 0, EXPERTS)
    perm_keys = jax.random.split(perm_key, GROUP_DEVS)
    ranks = jax.vmap(lambda one_key: jax.random.permutation(one_key, TOK_DEV))(perm_keys)
    flagged = ranks < TOK_DEV // 2
    is_hot = jnp.arange(EXPERTS)[None, None, :] == hot_ids[:, None, None]
    score = (noise + jnp.where(flagged[:, :, None] & is_hot, 1 << 21, 0)) * EXPERTS + jnp.arange(EXPERTS)[None, None, :]
    chosen = lax.top_k(score, TOP_K)[1]
    return chosen.astype(jnp.int32).reshape(GROUP_DEVS * SEQS_DEV, SEQ_LEN, TOP_K)


def setup_inputs(seed: int = 0, part: int = 0) -> dict:
    base_key = jax.random.key(seed)
    part_key = jax.random.fold_in(base_key, part)
    x_key, route_key, gate_key = jax.random.split(part_key, 3)
    weight_keys = jax.random.split(jax.random.key(seed + 1), 7)
    num_seqs = GROUP_DEVS * SEQS_DEV
    x = jax.random.normal(x_key, (num_seqs, SEQ_LEN, MODEL_DIM), jnp.float32).astype(jnp.bfloat16)
    expert_idx = draw_routing(route_key)
    gate = jax.random.uniform(gate_key, (num_seqs, SEQ_LEN, TOP_K), jnp.float32, 0.4, 1.6) * TOP_K ** -0.5
    attn_gain = jax.random.uniform(weight_keys[0], (MODEL_DIM,), jnp.float32, 0.5, 1.5)
    w_qkv = (jax.random.normal(weight_keys[1], (MODEL_DIM, QKV_HEADS, HEAD_DIM), jnp.float32) * (1.5 * MODEL_DIM ** -0.5)).astype(jnp.bfloat16)
    w_out = (jax.random.normal(weight_keys[2], (NUM_HEADS, HEAD_DIM, MODEL_DIM), jnp.float32) * (NUM_HEADS * HEAD_DIM) ** -0.5).astype(jnp.bfloat16)
    moe_gain = jax.random.uniform(weight_keys[3], (MODEL_DIM,), jnp.float32, 0.5, 1.5)
    w_gate = (jax.random.normal(weight_keys[4], (EXPERTS, MODEL_DIM, EXPERT_FF), jnp.float32) * MODEL_DIM ** -0.5).astype(jnp.bfloat16)
    w_up = (jax.random.normal(weight_keys[5], (EXPERTS, MODEL_DIM, EXPERT_FF), jnp.float32) * MODEL_DIM ** -0.5).astype(jnp.bfloat16)
    w_down = (jax.random.normal(weight_keys[6], (EXPERTS, EXPERT_FF, MODEL_DIM), jnp.float32) * (2.0 * EXPERT_FF ** -0.5)).astype(jnp.bfloat16)
    return {'x': x, 'expert_idx': expert_idx, 'gate': gate, 'attn_gain': attn_gain, 'w_qkv': w_qkv, 'w_out': w_out, 'moe_gain': moe_gain, 'w_gate': w_gate, 'w_up': w_up, 'w_down': w_down}


def rms_scale(tok_rows, gain):
    rows_f32 = tok_rows.astype(jnp.float32)
    inv_rms = lax.rsqrt(jnp.mean(rows_f32 * rows_f32, axis=-1, keepdims=True) + NORM_EPS)
    return (rows_f32 * inv_rms * gain).astype(jnp.bfloat16)


def apply_rope(head_vals):
    half_dim = HEAD_DIM // 2
    inv_freq = ROPE_BASE ** (-jnp.arange(half_dim, dtype=jnp.float32) * 2.0 / HEAD_DIM)
    angles = jnp.arange(SEQ_LEN, dtype=jnp.float32)[:, None] * inv_freq[None, :]
    cos_b = jnp.cos(angles)[:, None, :]
    sin_b = jnp.sin(angles)[:, None, :]
    vals_f32 = head_vals.astype(jnp.float32)
    low_half = vals_f32[..., :half_dim]
    high_half = vals_f32[..., half_dim:]
    return jnp.concatenate([low_half * cos_b - high_half * sin_b, high_half * cos_b + low_half * sin_b], axis=-1).astype(jnp.bfloat16)


def attend_one(seq_x, attn_gain, w_qkv, w_out):
    normed = rms_scale(seq_x, attn_gain)
    qkv_all = jnp.dot(normed, w_qkv.reshape(MODEL_DIM, QKV_HEADS * HEAD_DIM), preferred_element_type=jnp.float32).astype(jnp.bfloat16).reshape(SEQ_LEN, QKV_HEADS, HEAD_DIM)
    queries = apply_rope(qkv_all[:, :NUM_HEADS]).reshape(SEQ_LEN, KV_HEADS, GROUP_LEN, HEAD_DIM)
    keys_rot = apply_rope(qkv_all[:, NUM_HEADS:NUM_HEADS + KV_HEADS])
    values = qkv_all[:, NUM_HEADS + KV_HEADS:]
    scores = jnp.einsum('lkgd,mkd->kglm', queries.astype(jnp.float32), keys_rot.astype(jnp.float32)) * (HEAD_DIM ** -0.5)
    causal = jnp.arange(SEQ_LEN)[:, None] >= jnp.arange(SEQ_LEN)[None, :]
    attn_probs = jax.nn.softmax(jnp.where(causal, scores, -1e30), axis=-1).astype(jnp.bfloat16)
    mixed = jnp.einsum('kglm,mkd->lkgd', attn_probs.astype(jnp.float32), values.astype(jnp.float32)).astype(jnp.bfloat16)
    attn_proj = jnp.dot(mixed.reshape(SEQ_LEN, NUM_HEADS * HEAD_DIM), w_out.reshape(NUM_HEADS * HEAD_DIM, MODEL_DIM), preferred_element_type=jnp.float32)
    return (seq_x.astype(jnp.float32) + attn_proj).astype(jnp.bfloat16)


def dispatch_target(flat_ids):
    onehot = (flat_ids[:, None] == jnp.arange(EXPERTS)[None, :]).astype(jnp.int32)
    earlier = jnp.cumsum(onehot, axis=0) - onehot
    slot_pos = jnp.sum(earlier * onehot, axis=1)
    return jnp.where(slot_pos < CAPACITY, flat_ids * CAPACITY + slot_pos, EXPERTS * CAPACITY)


def run_expert(operands):
    tok_rows, gate_w, up_w, down_w = operands
    rows_f32 = tok_rows.astype(jnp.float32)
    act_gate = jnp.dot(rows_f32, gate_w.astype(jnp.float32))
    act_up = jnp.dot(rows_f32, up_w.astype(jnp.float32))
    mid_act = (jax.nn.silu(act_gate) * act_up).astype(jnp.bfloat16)
    return jnp.dot(mid_act.astype(jnp.float32), down_w.astype(jnp.float32)).astype(jnp.bfloat16)


def reference(x, expert_idx, gate, attn_gain, w_qkv, w_out, moe_gain, w_gate, w_up, w_down):
    hidden = lax.map(lambda seq_x: attend_one(seq_x, attn_gain, w_qkv, w_out), x)
    hid_dev = hidden.reshape(GROUP_DEVS, TOK_DEV, MODEL_DIM)
    ids_dev = expert_idx.reshape(GROUP_DEVS, TOK_DEV * TOP_K)
    gate_dev = gate.reshape(GROUP_DEVS, TOK_DEV, TOP_K)

    def build_buffer(operands):
        hid_rows, flat_ids = operands
        normed = rms_scale(hid_rows, moe_gain)
        target_rows = dispatch_target(flat_ids)
        filled = jnp.zeros((EXPERTS * CAPACITY + 1, MODEL_DIM), jnp.bfloat16).at[target_rows].set(jnp.repeat(normed, TOP_K, axis=0))
        return filled[:EXPERTS * CAPACITY].reshape(EXPERTS, CAPACITY, MODEL_DIM), target_rows

    buffers, target_all = lax.map(build_buffer, (hid_dev, ids_dev))
    by_expert = jnp.transpose(buffers, (1, 0, 2, 3)).reshape(EXPERTS, GROUP_DEVS * CAPACITY, MODEL_DIM)
    expert_out = lax.map(run_expert, (by_expert, w_gate, w_up, w_down))
    out_dev = jnp.transpose(expert_out.reshape(EXPERTS, GROUP_DEVS, CAPACITY, MODEL_DIM), (1, 0, 2, 3)).reshape(GROUP_DEVS, EXPERTS * CAPACITY, MODEL_DIM)

    def combine(operands):
        hid_rows, out_rows, target_rows, gate_rows = operands
        padded = jnp.concatenate([out_rows, jnp.zeros((1, MODEL_DIM), jnp.bfloat16)], axis=0)
        picked = jnp.take(padded, target_rows, axis=0).reshape(TOK_DEV, TOP_K, MODEL_DIM).astype(jnp.float32)
        total = hid_rows.astype(jnp.float32) + jnp.sum(picked * gate_rows[:, :, None], axis=1)
        return total.astype(jnp.bfloat16)

    result = lax.map(combine, (hid_dev, out_dev, target_all, gate_dev))
    return result.reshape(GROUP_DEVS * SEQS_DEV, SEQ_LEN, MODEL_DIM)
```

```python
import functools

import jax
import jax.numpy as jnp
from jax import lax
from jax.experimental import pallas as pl
from jax.experimental.pallas import tpu as pltpu
from jax.sharding import PartitionSpec as P

NORM_EPS = 1e-6
ROPE_BASE = 10000.0


def rms_scale(tok_rows, gain):
    rows_f32 = tok_rows.astype(jnp.float32)
    inv_rms = lax.rsqrt(jnp.mean(rows_f32 * rows_f32, axis=-1, keepdims=True) + NORM_EPS)
    return (rows_f32 * inv_rms * gain).astype(jnp.bfloat16)


def rope_apply(head_vals):
    seq_len, head_dim = head_vals.shape[1], head_vals.shape[-1]
    half_dim = head_dim // 2
    inv_freq = ROPE_BASE ** (-jnp.arange(half_dim, dtype=jnp.float32) * 2.0 / head_dim)
    angles = jnp.arange(seq_len, dtype=jnp.float32)[:, None] * inv_freq[None, :]
    cos_b = jnp.cos(angles)[None, :, None, :]
    sin_b = jnp.sin(angles)[None, :, None, :]
    vals_f32 = head_vals.astype(jnp.float32)
    low_half = vals_f32[..., :half_dim]
    high_half = vals_f32[..., half_dim:]
    return jnp.concatenate([low_half * cos_b - high_half * sin_b, high_half * cos_b + low_half * sin_b], axis=-1).astype(jnp.bfloat16)


def attention_block(seqs, attn_gain, w_qkv, w_out_t, num_heads, head_dim):
    num_seqs, seq_len, model_dim = seqs.shape
    normed = rms_scale(seqs, attn_gain).reshape(num_seqs * seq_len, model_dim)
    qkv = jnp.dot(normed, w_qkv, preferred_element_type=jnp.float32).astype(jnp.bfloat16)
    qkv_all = qkv.reshape(num_seqs, seq_len, -1, head_dim)
    kv_heads = qkv_all.shape[2] - 2 * num_heads
    queries = rope_apply(qkv_all[:, :, :num_heads])
    keys_rot = rope_apply(qkv_all[:, :, num_heads:num_heads + kv_heads])
    values = qkv_all[:, :, num_heads + kv_heads:]
    scores = jnp.einsum('slkd,smkd->sklm', queries, keys_rot, preferred_element_type=jnp.float32) * (head_dim ** -0.5)
    causal = lax.broadcasted_iota(jnp.int32, (seq_len, seq_len), 0) >= lax.broadcasted_iota(jnp.int32, (seq_len, seq_len), 1)
    attn_probs = jax.nn.softmax(jnp.where(causal, scores, -1e30), axis=-1).astype(jnp.bfloat16)
    mixed = jnp.einsum('sklm,smkd->slkd', attn_probs, values, preferred_element_type=jnp.float32).astype(jnp.bfloat16)
    attn_proj = lax.dot_general(mixed.reshape(num_seqs * seq_len, num_heads * head_dim), w_out_t, (((1,), (1,)), ((), ())), preferred_element_type=jnp.float32)
    return (seqs.reshape(num_seqs * seq_len, model_dim).astype(jnp.float32) + attn_proj).astype(jnp.bfloat16)


def capacity_of(tok_dev, top_k, num_experts):
    return 8 * ((5 * top_k * tok_dev + 32 * num_experts - 1) // (32 * num_experts))


def slots_of(flat_ids, num_experts):
    onehot = (flat_ids[:, None] == jnp.arange(num_experts, dtype=jnp.int32)[None, :]).astype(jnp.int32)
    earlier = jnp.cumsum(onehot, axis=0) - onehot
    return jnp.sum(earlier * onehot, axis=1)


def tile_of(size, most):
    return max(t for t in range(128, most + 1, 128) if size % t == 0)


def up_kernel(ids_ref, z_a, z_b, wg_a, wg_b, wu_a, wu_b, mid_ref):
    ff = mid_ref.shape[1]
    w_a = jnp.concatenate([wg_a[0], wu_a[0]], axis=1)
    w_b = jnp.concatenate([wg_b[0], wu_b[0]], axis=1)
    w = jnp.concatenate([w_a, w_b], axis=0)
    rows = mid_ref.shape[0]
    start = pl.multiple_of(pl.program_id(1) * rows, rows)
    z = jnp.concatenate([z_a[pl.ds(start, rows), :], z_b[pl.ds(start, rows), :]], axis=1)
    acc = jnp.dot(z, w, preferred_element_type=jnp.float32)
    act_gate = acc[:, :ff]
    mid_ref[...] = (act_gate * jax.nn.sigmoid(act_gate) * acc[:, ff:]).astype(mid_ref.dtype)


def expert_up(ids, z, wg_own, wg_got, wu_own, wu_got):
    rows, model_dim = z.shape
    half = model_dim // 2
    ff_dim = wg_own.shape[2]
    ff = tile_of(ff_dim, 384)
    rb = tile_of(rows, 1280)
    own = pl.BlockSpec((1, half, ff), lambda j, i, s: (s[0], 0, j))
    got = pl.BlockSpec((1, half, ff), lambda j, i, s: (1 - s[0], 0, j))
    once = pl.Buffered(buffer_count=1)
    return pl.pallas_call(
        up_kernel,
        grid_spec=pltpu.PrefetchScalarGridSpec(
            num_scalar_prefetch=1,
            grid=(ff_dim // ff, rows // rb),
            in_specs=[
                pl.BlockSpec((rows, half), lambda j, i, s: (0, s[0]), pipeline_mode=once),
                pl.BlockSpec((rows, half), lambda j, i, s: (0, 1 - s[0]), pipeline_mode=once),
                own, got, own, got,
            ],
            out_specs=pl.BlockSpec((rb, ff), lambda j, i, s: (i, j)),
        ),
        out_shape=jax.ShapeDtypeStruct((rows, ff_dim), jnp.bfloat16),
        compiler_params=pltpu.CompilerParams(dimension_semantics=("arbitrary", "arbitrary"), vmem_limit_bytes=60 * 2**20),
        cost_estimate=pl.CostEstimate(flops=4 * rows * model_dim * ff_dim, bytes_accessed=2 * (rows * model_dim + 2 * model_dim * ff_dim + rows * ff_dim), transcendentals=rows * ff_dim),
        name="expert_up",
    )(ids, z, z, wg_own, wg_got, wu_own, wu_got)


def down_kernel(ids_ref, mid_ref, w_a, w_b, out_ref):
    half = w_a.shape[2]
    w = jnp.concatenate([w_a[0], w_b[0]], axis=1)
    acc = jnp.dot(mid_ref[...], w, preferred_element_type=jnp.float32)
    first = ids_ref[0] == 0
    own, got = acc[:, :half], acc[:, half:]
    out_ref[:, :half] = jnp.where(first, own, got).astype(out_ref.dtype)
    out_ref[:, half:] = jnp.where(first, got, own).astype(out_ref.dtype)


def expert_down(ids, mid, w_own, w_got):
    rows, ff_dim = mid.shape
    half = w_own.shape[2]
    rb = tile_of(rows, 320) if rows % 256 else 256
    once = pl.Buffered(buffer_count=1)
    return pl.pallas_call(
        down_kernel,
        grid_spec=pltpu.PrefetchScalarGridSpec(
            num_scalar_prefetch=1,
            grid=(rows // rb,),
            in_specs=[
                pl.BlockSpec((rb, ff_dim), lambda i, s: (i, 0)),
                pl.BlockSpec((1, ff_dim, half), lambda i, s: (s[0], 0, 0), pipeline_mode=once),
                pl.BlockSpec((1, ff_dim, half), lambda i, s: (1 - s[0], 0, 0), pipeline_mode=once),
            ],
            out_specs=pl.BlockSpec((rb, 2 * half), lambda i, s: (i, 0)),
        ),
        out_shape=jax.ShapeDtypeStruct((rows, 2 * half), jnp.bfloat16),
        compiler_params=pltpu.CompilerParams(dimension_semantics=("arbitrary",), vmem_limit_bytes=60 * 2**20),
        cost_estimate=pl.CostEstimate(flops=4 * rows * half * ff_dim, bytes_accessed=2 * (2 * rows * half + 2 * half * ff_dim + rows * ff_dim), transcendentals=0),
        name="expert_down",
    )(ids, mid, w_own, w_got)


def solution(mesh):
    tok_spec = P(('rep', 'expert', 'data'), None, None)
    group_axes = ('data', 'expert')
    token_axes = ('expert', 'data')
    num_experts = mesh.shape['expert'] * mesh.shape['data']

    def local_step(x_loc, idx_loc, gate_loc, attn_gain, qkv_part, out_part, moe_gain, gate_part, up_part, down_part):
        num_seqs, seq_len, model_dim = x_loc.shape
        num_heads, head_dim = out_part.shape[0], out_part.shape[1]
        tok_dev = num_seqs * seq_len
        top_k = idx_loc.shape[-1]
        capacity = capacity_of(tok_dev, top_k, num_experts)
        mine = lax.axis_index('data')
        ids = jnp.stack([mine]).astype(jnp.int32)

        w_qkv = lax.all_gather(qkv_part.reshape(qkv_part.shape[0], -1), group_axes, axis=0, tiled=True)
        w_out_t = lax.all_gather(out_part.reshape(num_heads * head_dim, -1).T, group_axes, axis=0, tiled=True)

        def swap(part):
            return lax.all_gather(lax.dynamic_index_in_dim(part, 1 - mine, 0, keepdims=False), 'data')

        got_gate, got_up, got_down = swap(gate_part), swap(up_part), swap(down_part)

        flat_ids = idx_loc.reshape(tok_dev * top_k)
        slot_pos = slots_of(flat_ids, num_experts)
        kept = slot_pos < capacity
        target = flat_ids * capacity + slot_pos
        source = jnp.zeros((num_experts * capacity,), jnp.int32)
        source = source.at[jnp.where(kept, target, num_experts * capacity)].set(jnp.arange(tok_dev * top_k, dtype=jnp.int32) // top_k, mode='drop', unique_indices=False)

        hidden = attention_block(x_loc, attn_gain, w_qkv, w_out_t, num_heads, head_dim)
        normed = rms_scale(hidden, moe_gain)
        send = normed.at[source].get(mode='promise_in_bounds')
        rows = lax.all_to_all(send.reshape(num_experts, capacity, model_dim), token_axes, 0, 0, tiled=True)
        mid = expert_up(ids, rows.reshape(num_experts * capacity, model_dim), gate_part, got_gate, up_part, got_up)
        outs = expert_down(ids, mid, down_part, got_down)
        back = lax.all_to_all(outs.reshape(num_experts, capacity, model_dim), token_axes, 0, 0, tiled=True).reshape(num_experts * capacity, model_dim)
        pick = jnp.where(kept, target, 0).reshape(tok_dev, top_k)
        kept = kept.reshape(tok_dev, top_k)
        gates = gate_loc.reshape(tok_dev, top_k)
        mixed = None
        for k in range(top_k):
            got = back.at[pick[:, k]].get(mode='promise_in_bounds').astype(jnp.float32)
            term = jnp.where(kept[:, k, None], got * gates[:, k, None], 0.0)
            mixed = term if mixed is None else mixed + term
        total = hidden.astype(jnp.float32) + mixed
        return total.astype(jnp.bfloat16).reshape(num_seqs, seq_len, model_dim)

    in_specs = (tok_spec, tok_spec, tok_spec, P(None), P(group_axes, None, None), P(None, None, group_axes), P(None), P('expert', 'data', None), P('expert', 'data', None), P('expert', None, 'data'))
    return jax.shard_map(local_step, mesh=mesh, in_specs=in_specs, out_specs=tok_spec, check_vma=False)
```

```python
import functools

import jax
import jax.numpy as jnp
from jax import lax
from jax.experimental import pallas as pl
from jax.experimental.pallas import tpu as pltpu
from jax.sharding import PartitionSpec as P

NORM_EPS = 1e-6
ROPE_BASE = 10000.0


def rms_scale(tok_rows, gain):
    rows_f32 = tok_rows.astype(jnp.float32)
    inv_rms = lax.rsqrt(jnp.mean(rows_f32 * rows_f32, axis=-1, keepdims=True) + NORM_EPS)
    return (rows_f32 * inv_rms * gain).astype(jnp.bfloat16)


def rope_tables(seq_len, head_dim, lanes):
    half_dim = head_dim // 2
    inv_freq = ROPE_BASE ** (-jnp.arange(half_dim, dtype=jnp.float32) * 2.0 / head_dim)
    angles = jnp.arange(seq_len, dtype=jnp.float32)[:, None] * inv_freq[None, :]
    cos_b, sin_b = jnp.cos(angles), jnp.sin(angles)
    times = lanes // head_dim
    return jnp.tile(jnp.concatenate([cos_b, cos_b], axis=1), (1, times)), jnp.tile(jnp.concatenate([-sin_b, sin_b], axis=1), (1, times))


def attention_kernel(head_dim, num_heads, qkv_ref, cos_ref, sin_ref, out_ref):
    seq_len = qkv_ref.shape[0]
    lanes = cos_ref.shape[1]
    per_block = lanes // head_dim
    width = num_heads * head_dim
    lane = lax.broadcasted_iota(jnp.int32, (seq_len, lanes), 1)
    low = lane % head_dim < head_dim // 2
    row_id = lax.broadcasted_iota(jnp.int32, (seq_len, seq_len), 0)
    causal = row_id >= lax.broadcasted_iota(jnp.int32, (seq_len, seq_len), 1)
    causal = jnp.concatenate([causal] * per_block, axis=0)
    cos_b, sin_b = cos_ref[...], sin_ref[...]

    def rope(vals):
        vals = vals.astype(jnp.float32)
        turned = jnp.where(low, pltpu.roll(vals, lanes - head_dim // 2, 1), pltpu.roll(vals, head_dim // 2, 1))
        return vals * cos_b + turned * sin_b

    for start in range(0, width, lanes):
        queries = rope(qkv_ref[:, start:start + lanes])
        keys = rope(qkv_ref[:, width + start:width + start + lanes]).astype(jnp.bfloat16)
        values = qkv_ref[:, 2 * width + start:2 * width + start + lanes]
        stacked = jnp.concatenate([jnp.where(lane // head_dim == h, queries, 0.0) for h in range(per_block)], axis=0).astype(jnp.bfloat16)
        scores = lax.dot_general(stacked, keys, (((1,), (1,)), ((), ())), preferred_element_type=jnp.float32) * (head_dim ** -0.5)
        scores = jnp.where(causal, scores, -1e30)
        weights = jnp.exp(scores - jnp.max(scores, axis=1, keepdims=True))
        probs = (weights / jnp.sum(weights, axis=1, keepdims=True)).astype(jnp.bfloat16)
        mixed = jnp.dot(probs, values, preferred_element_type=jnp.float32)
        out = mixed[:seq_len]
        for h in range(1, per_block):
            out = jnp.where(lane // head_dim == h, mixed[h * seq_len:(h + 1) * seq_len], out)
        out_ref[:, start:start + lanes] = out.astype(out_ref.dtype)


def attention_core(qkv, num_seqs, num_heads, head_dim):
    rows, width = qkv.shape
    seq_len = rows // num_seqs
    lanes = 128
    cos_b, sin_b = rope_tables(seq_len, head_dim, lanes)
    table = pl.BlockSpec((seq_len, lanes), lambda i: (0, 0))
    return pl.pallas_call(
        functools.partial(attention_kernel, head_dim, num_heads),
        grid=(num_seqs,),
        in_specs=[pl.BlockSpec((seq_len, width), lambda i: (i, 0)), table, table],
        out_specs=pl.BlockSpec((seq_len, width // 3), lambda i: (i, 0)),
        out_shape=jax.ShapeDtypeStruct((rows, width // 3), jnp.bfloat16),
        compiler_params=pltpu.CompilerParams(dimension_semantics=("arbitrary",), vmem_limit_bytes=32 * 2**20),
        cost_estimate=pl.CostEstimate(flops=40 * 10**9, bytes_accessed=8 * rows * width // 3, transcendentals=rows * seq_len * num_heads),
        name="attention_core",
    )(qkv, cos_b, sin_b)


def attention_block(seqs, attn_gain, w_qkv, w_out_t, num_heads, head_dim):
    num_seqs, seq_len, model_dim = seqs.shape
    normed = rms_scale(seqs, attn_gain).reshape(num_seqs * seq_len, model_dim)
    qkv = jnp.dot(normed, w_qkv, preferred_element_type=jnp.float32).astype(jnp.bfloat16)
    mixed = attention_core(qkv, num_seqs, num_heads, head_dim)
    attn_proj = lax.dot_general(mixed, w_out_t, (((1,), (1,)), ((), ())), preferred_element_type=jnp.float32)
    return (seqs.reshape(num_seqs * seq_len, model_dim).astype(jnp.float32) + attn_proj).astype(jnp.bfloat16)


def capacity_of(tok_dev, top_k, num_experts):
    return 8 * ((5 * top_k * tok_dev + 32 * num_experts - 1) // (32 * num_experts))


def slots_of(flat_ids, num_experts):
    onehot = (flat_ids[:, None] == jnp.arange(num_experts, dtype=jnp.int32)[None, :]).astype(jnp.int32)
    earlier = jnp.cumsum(onehot, axis=0) - onehot
    return jnp.sum(earlier * onehot, axis=1)


def tile_of(size, most):
    return max(t for t in range(128, most + 1, 128) if size % t == 0)


def up_kernel(ids_ref, z_a, z_b, wg_a, wg_b, wu_a, wu_b, mid_ref):
    ff = mid_ref.shape[1]
    w_a = jnp.concatenate([wg_a[0], wu_a[0]], axis=1)
    w_b = jnp.concatenate([wg_b[0], wu_b[0]], axis=1)
    w = jnp.concatenate([w_a, w_b], axis=0)
    rows = mid_ref.shape[0]
    start = pl.multiple_of(pl.program_id(1) * rows, rows)
    z = jnp.concatenate([z_a[pl.ds(start, rows), :], z_b[pl.ds(start, rows), :]], axis=1)
    acc = jnp.dot(z, w, preferred_element_type=jnp.float32)
    act_gate = acc[:, :ff]
    mid_ref[...] = (act_gate * jax.nn.sigmoid(act_gate) * acc[:, ff:]).astype(mid_ref.dtype)


def expert_up(ids, z, wg_own, wu_own, wg_got, wu_got, first, ff_dim, ff):
    rows, model_dim = z.shape
    half = model_dim // 2
    rb = tile_of(rows, 1280)
    tiles = ff_dim // ff
    own = pl.BlockSpec((1, half, ff), lambda j, i, s: (s[0], 0, first // ff + j))
    got = pl.BlockSpec((1, half, ff), lambda j, i, s: (1 - s[0], 0, j))
    once = pl.Buffered(buffer_count=1)
    return pl.pallas_call(
        up_kernel,
        grid_spec=pltpu.PrefetchScalarGridSpec(
            num_scalar_prefetch=1,
            grid=(tiles, rows // rb),
            in_specs=[
                pl.BlockSpec((rows, half), lambda j, i, s: (0, s[0]), pipeline_mode=once),
                pl.BlockSpec((rows, half), lambda j, i, s: (0, 1 - s[0]), pipeline_mode=once),
                own, got, own, got,
            ],
            out_specs=pl.BlockSpec((rb, ff), lambda j, i, s: (i, j)),
        ),
        out_shape=jax.ShapeDtypeStruct((rows, ff_dim), jnp.bfloat16),
        compiler_params=pltpu.CompilerParams(dimension_semantics=("arbitrary", "arbitrary"), vmem_limit_bytes=60 * 2**20),
        cost_estimate=pl.CostEstimate(flops=4 * rows * model_dim * ff_dim, bytes_accessed=2 * (rows * model_dim + 2 * model_dim * ff_dim + rows * ff_dim), transcendentals=rows * ff_dim),
        name="expert_up",
    )(ids, z, z, wg_own, wg_got, wu_own, wu_got)


def down_kernel(ids_ref, mid_a, mid_b, *refs):
    out_ref = refs[-1]
    w = [r[0] if len(r.shape) == 3 else r[...] for r in refs[:-1]]
    w = w[0] if len(w) == 1 else jnp.concatenate(w, axis=1)
    mid = jnp.concatenate([mid_a[...], mid_b[...]], axis=1)
    out_ref[...] = jnp.dot(mid, w, preferred_element_type=jnp.float32).astype(out_ref.dtype)


def expert_down(ids, mids, weights, specs, cols, name):
    rows = mids[0].shape[0]
    ff_dim = sum(m.shape[1] for m in mids)
    rb = tile_of(rows, 512)
    return pl.pallas_call(
        down_kernel,
        grid_spec=pltpu.PrefetchScalarGridSpec(
            num_scalar_prefetch=1,
            grid=(rows // rb,),
            in_specs=[pl.BlockSpec((rb, m.shape[1]), lambda i, s: (i, 0)) for m in mids] + specs,
            out_specs=pl.BlockSpec((rb, cols), lambda i, s: (i, 0)),
        ),
        out_shape=jax.ShapeDtypeStruct((rows, cols), jnp.bfloat16),
        compiler_params=pltpu.CompilerParams(dimension_semantics=("arbitrary",), vmem_limit_bytes=60 * 2**20),
        cost_estimate=pl.CostEstimate(flops=2 * rows * cols * ff_dim, bytes_accessed=2 * (rows * cols + cols * ff_dim + rows * ff_dim), transcendentals=0),
        name=name,
    )(ids, *mids, *weights)


def solution(mesh):
    tok_spec = P(('rep', 'expert', 'data'), None, None)
    group_axes = ('data', 'expert')
    token_axes = ('expert', 'data')
    data_size, expert_size = mesh.shape['data'], mesh.shape['expert']
    num_experts = expert_size * data_size
    other_data = [(0, 1), (1, 0)]
    other_chip = [(e, e ^ 2) for e in range(expert_size)]
    other_core = [(e, e ^ 1) for e in range(expert_size)]

    def local_step(x_loc, idx_loc, gate_loc, attn_gain, qkv_part, out_part, moe_gain, gate_part, up_part, down_part):
        num_seqs, seq_len, model_dim = x_loc.shape
        num_heads, head_dim = out_part.shape[0], out_part.shape[1]
        tok_dev = num_seqs * seq_len
        top_k = idx_loc.shape[-1]
        capacity = capacity_of(tok_dev, top_k, num_experts)
        half, ff_dim = gate_part.shape[1:]
        mine = lax.axis_index('data')
        place = lax.axis_index('expert')
        ids = jnp.stack([mine]).astype(jnp.int32)

        def spread(part):
            along = lax.ppermute(part, 'data', other_data)
            own = [part, lax.ppermute(part, 'expert', other_chip)]
            peer = [along, lax.ppermute(along, 'expert', other_chip)]
            whole = jnp.zeros((data_size, expert_size) + part.shape, part.dtype)
            for row, pieces in ((mine, own), (1 - mine, peer)):
                for chip, piece in enumerate(pieces):
                    there = place ^ (2 * chip)
                    whole = lax.dynamic_update_slice(whole, piece[None, None], (row, there, 0, 0))
                    whole = lax.dynamic_update_slice(whole, lax.ppermute(piece, 'expert', other_core)[None, None], (row, there ^ 1, 0, 0))
            return whole.reshape(-1, part.shape[1]), (along, own[1])

        w_qkv, ahead = spread(qkv_part.reshape(qkv_part.shape[0], -1))

        theirs = 1 - mine
        ff = tile_of(ff_dim, 384)
        split = ff_dim // ff // 2 * ff
        cuts = ((0, split), (split, ff_dim - split))
        sends = [lax.dynamic_slice(p, (theirs, 0, first), (1, half, size))[0] for first, size in cuts for p in (gate_part, up_part)]
        out_t = out_part.reshape(num_heads * head_dim, -1).T
        sends, _ = lax.optimization_barrier((sends, ahead))
        out_t, w_qkv = lax.optimization_barrier((out_t, w_qkv))
        w_out_t, _ = spread(out_t)
        got = [lax.all_gather(part, 'data') for part in sends]
        got_up = [got[:2], got[2:]]

        flat_ids = idx_loc.reshape(tok_dev * top_k)
        slot_pos = slots_of(flat_ids, num_experts)
        kept = slot_pos < capacity
        target = flat_ids * capacity + slot_pos
        source = jnp.zeros((num_experts * capacity,), jnp.int32)
        source = source.at[jnp.where(kept, target, num_experts * capacity)].set(jnp.arange(tok_dev * top_k, dtype=jnp.int32) // top_k, mode='drop', unique_indices=False)

        hidden = attention_block(x_loc, attn_gain, w_qkv, w_out_t, num_heads, head_dim)
        normed = rms_scale(hidden, moe_gain)
        send = normed.at[source].get(mode='promise_in_bounds')
        rows = lax.all_to_all(send.reshape(num_experts, capacity, model_dim), token_axes, 0, 0, tiled=True)
        down_send, rows = lax.optimization_barrier((lax.dynamic_index_in_dim(down_part, theirs, 0, keepdims=False), rows))
        got_down = lax.ppermute(down_send, 'data', other_data)
        rows = rows.reshape(num_experts * capacity, model_dim)
        mids = [expert_up(ids, rows, gate_part, up_part, *pair, first, size, ff) for pair, (first, size) in zip(got_up, cuts)]

        early = half // 256 * 256
        late = 2 * half - early
        once = pl.Buffered(buffer_count=1)

        def back(cols):
            return lax.all_to_all(cols.reshape(num_experts, capacity, -1), token_axes, 0, 0, tiled=True).reshape(num_experts * capacity, -1)

        spec_early = pl.BlockSpec((1, ff_dim, early), lambda i, s: (s[0], 0, 0), pipeline_mode=once)
        spec_rest = pl.BlockSpec((1, ff_dim, half - early), lambda i, s: (s[0], 0, early // (half - early)), pipeline_mode=once)
        spec_got = pl.BlockSpec((ff_dim, half), lambda i, s: (0, 0), pipeline_mode=once)
        pieces = [
            back(expert_down(ids, mids, [down_part], [spec_early], early, "expert_down_own")),
            back(expert_down(ids, mids, [down_part, got_down], [spec_rest, spec_got], late, "expert_down_got")),
        ]

        pick = jnp.where(kept, target, 0).reshape(tok_dev, top_k)
        odd = (flat_ids % data_size == 1).reshape(tok_dev, top_k)
        kept = kept.reshape(tok_dev, top_k)
        gates = gate_loc.reshape(tok_dev, top_k)
        mixed = [None, None]
        for k in range(top_k):
            got = [p.at[pick[:, k]].get(mode='promise_in_bounds') for p in pieces]
            own, rest = jnp.concatenate([got[0], got[1][:, :half - early]], axis=1), got[1][:, half - early:]
            flip = odd[:, k, None]
            for side, value in enumerate((jnp.where(flip, rest, own), jnp.where(flip, own, rest))):
                term = jnp.where(kept[:, k, None], value.astype(jnp.float32) * gates[:, k, None], 0.0)
                mixed[side] = term if mixed[side] is None else mixed[side] + term
        total = hidden.astype(jnp.float32) + jnp.concatenate(mixed, axis=1)
        return total.astype(jnp.bfloat16).reshape(num_seqs, seq_len, model_dim)

    in_specs = (tok_spec, tok_spec, tok_spec, P(None), P(group_axes, None, None), P(None, None, group_axes), P(None), P('expert', 'data', None), P('expert', 'data', None), P('expert', None, 'data'))
    return jax.shard_map(local_step, mesh=mesh, in_specs=in_specs, out_specs=tok_spec, check_vma=False)
```

```python
import functools

import jax
import jax.numpy as jnp
from jax import lax
from jax.experimental import pallas as pl
from jax.experimental.pallas import tpu as pltpu
from jax.sharding import PartitionSpec as P

NORM_EPS = 1e-6
ROPE_BASE = 10000.0


def rms_scale(tok_rows, gain):
    rows_f32 = tok_rows.astype(jnp.float32)
    inv_rms = lax.rsqrt(jnp.mean(rows_f32 * rows_f32, axis=-1, keepdims=True) + NORM_EPS)
    return (rows_f32 * inv_rms * gain).astype(jnp.bfloat16)


def rope_tables(seq_len, head_dim, lanes):
    half_dim = head_dim // 2
    inv_freq = ROPE_BASE ** (-jnp.arange(half_dim, dtype=jnp.float32) * 2.0 / head_dim)
    angles = jnp.arange(seq_len, dtype=jnp.float32)[:, None] * inv_freq[None, :]
    cos_b, sin_b = jnp.cos(angles), jnp.sin(angles)
    times = lanes // head_dim
    return jnp.tile(jnp.concatenate([cos_b, cos_b], axis=1), (1, times)), jnp.tile(jnp.concatenate([-sin_b, sin_b], axis=1), (1, times))


def attention_kernel(head_dim, num_heads, qkv_ref, cos_ref, sin_ref, out_ref):
    seq_len = qkv_ref.shape[0]
    lanes = cos_ref.shape[1]
    per_block = lanes // head_dim
    width = num_heads * head_dim
    lane = lax.broadcasted_iota(jnp.int32, (seq_len, lanes), 1)
    low = lane % head_dim < head_dim // 2
    row_id = lax.broadcasted_iota(jnp.int32, (seq_len, seq_len), 0)
    causal = row_id >= lax.broadcasted_iota(jnp.int32, (seq_len, seq_len), 1)
    causal = jnp.concatenate([causal] * per_block, axis=0)
    cos_b, sin_b = cos_ref[...], sin_ref[...]

    def rope(vals):
        vals = vals.astype(jnp.float32)
        turned = jnp.where(low, pltpu.roll(vals, lanes - head_dim // 2, 1), pltpu.roll(vals, head_dim // 2, 1))
        return vals * cos_b + turned * sin_b

    for start in range(0, width, lanes):
        queries = rope(qkv_ref[:, start:start + lanes])
        keys = rope(qkv_ref[:, width + start:width + start + lanes]).astype(jnp.bfloat16)
        values = qkv_ref[:, 2 * width + start:2 * width + start + lanes]
        stacked = jnp.concatenate([jnp.where(lane // head_dim == h, queries, 0.0) for h in range(per_block)], axis=0).astype(jnp.bfloat16)
        scores = lax.dot_general(stacked, keys, (((1,), (1,)), ((), ())), preferred_element_type=jnp.float32) * (head_dim ** -0.5)
        scores = jnp.where(causal, scores, -1e30)
        weights = jnp.exp(scores - jnp.max(scores, axis=1, keepdims=True))
        probs = (weights / jnp.sum(weights, axis=1, keepdims=True)).astype(jnp.bfloat16)
        mixed = jnp.dot(probs, values, preferred_element_type=jnp.float32)
        out = mixed[:seq_len]
        for h in range(1, per_block):
            out = jnp.where(lane // head_dim == h, mixed[h * seq_len:(h + 1) * seq_len], out)
        out_ref[:, start:start + lanes] = out.astype(out_ref.dtype)


def attention_core(qkv, num_seqs, num_heads, head_dim):
    rows, width = qkv.shape
    seq_len = rows // num_seqs
    lanes = 128
    cos_b, sin_b = rope_tables(seq_len, head_dim, lanes)
    table = pl.BlockSpec((seq_len, lanes), lambda i: (0, 0))
    return pl.pallas_call(
        functools.partial(attention_kernel, head_dim, num_heads),
        grid=(num_seqs,),
        in_specs=[pl.BlockSpec((seq_len, width), lambda i: (i, 0)), table, table],
        out_specs=pl.BlockSpec((seq_len, width // 3), lambda i: (i, 0)),
        out_shape=jax.ShapeDtypeStruct((rows, width // 3), jnp.bfloat16),
        compiler_params=pltpu.CompilerParams(dimension_semantics=("arbitrary",), vmem_limit_bytes=32 * 2**20),
        cost_estimate=pl.CostEstimate(flops=40 * 10**9, bytes_accessed=8 * rows * width // 3, transcendentals=rows * seq_len * num_heads),
        name="attention_core",
    )(qkv, cos_b, sin_b)


def capacity_of(tok_dev, top_k, num_experts):
    return 8 * ((5 * top_k * tok_dev + 32 * num_experts - 1) // (32 * num_experts))


def slots_of(flat_ids, num_experts):
    onehot = (flat_ids[:, None] == jnp.arange(num_experts, dtype=jnp.int32)[None, :]).astype(jnp.int32)
    earlier = jnp.cumsum(onehot, axis=0) - onehot
    return jnp.sum(earlier * onehot, axis=1)


def tile_of(size, most):
    return max(t for t in range(128, most + 1, 128) if size % t == 0)


def up_kernel(ids_ref, z_a, z_b, wg_a, wg_b, wu_a, wu_b, *refs):
    mid_ref = refs[-1]
    ff = mid_ref.shape[1]
    w_a = jnp.concatenate([wg_a[0], wu_a[0]], axis=1)
    w_b = jnp.concatenate([wg_b[0], wu_b[0]], axis=1)
    w = jnp.concatenate([w_a, w_b], axis=0)
    rows = mid_ref.shape[0]
    start = pl.multiple_of(pl.program_id(1) * rows, rows)
    z = jnp.concatenate([z_a[pl.ds(start, rows), :], z_b[pl.ds(start, rows), :]], axis=1)
    acc = jnp.dot(z, w, preferred_element_type=jnp.float32)
    act_gate = acc[:, :ff]
    mid_ref[...] = (act_gate * jax.nn.sigmoid(act_gate) * acc[:, ff:]).astype(mid_ref.dtype)


def expert_up(ids, z, wg_own, wg_got, wu_own, wu_got, mid, first, ff, capacity, peer):
    rows, model_dim = z.shape
    half = model_dim // 2
    size, ff_dim = wg_got.shape[2], wg_own.shape[2]
    tiles, skip = size // ff, first // ff
    own = pl.BlockSpec((1, half, ff), lambda j, i, s: (s[0], 0, skip + j))
    got = pl.BlockSpec((1, half, ff), lambda j, i, s: (0 if wg_got.shape[0] == 1 else 1 - s[0], 0, j))
    once = pl.Buffered(buffer_count=1)
    given = [] if mid is None else [mid]
    return pl.pallas_call(
        up_kernel,
        grid_spec=pltpu.PrefetchScalarGridSpec(
            num_scalar_prefetch=1,
            grid=(tiles, rows // capacity),
            in_specs=[
                pl.BlockSpec((rows, half), lambda j, i, s: (0, s[0]), pipeline_mode=once),
                pl.BlockSpec((rows, half), lambda j, i, s: (0, 1 - s[0]), pipeline_mode=once),
                own, got, own, got,
            ] + [pl.BlockSpec(memory_space=pl.ANY)] * len(given),
            out_specs=pl.BlockSpec((capacity, ff), lambda j, i, s: (2 * i + (1 - s[0] if peer else s[0]), skip + j)),
        ),
        out_shape=jax.ShapeDtypeStruct((2 * rows, ff_dim), jnp.bfloat16),
        input_output_aliases={7: 0} if given else {},
        compiler_params=pltpu.CompilerParams(dimension_semantics=("arbitrary", "arbitrary"), vmem_limit_bytes=48 * 2**20),
        cost_estimate=pl.CostEstimate(flops=4 * rows * model_dim * size, bytes_accessed=2 * (rows * model_dim + 2 * model_dim * size + rows * size), transcendentals=rows * size),
        name="expert_up",
    )(ids, z, z, wg_own, wg_got, wu_own, wu_got, *given)


def down_kernel(ids_ref, mid_ref, *refs):
    out_ref = refs[-1]
    w = [r[0] if len(r.shape) == 3 else r[...] for r in refs[:-1]]
    w = w[0] if len(w) == 1 else jnp.concatenate(w, axis=1)
    out_ref[...] = jnp.dot(mid_ref[...], w, preferred_element_type=jnp.float32).astype(out_ref.dtype)


def expert_down(ids, mid, weights, specs, cols, name):
    rows, ff_dim = mid.shape
    rb = tile_of(rows, 512)
    return pl.pallas_call(
        down_kernel,
        grid_spec=pltpu.PrefetchScalarGridSpec(
            num_scalar_prefetch=1,
            grid=(rows // rb,),
            in_specs=[pl.BlockSpec((rb, ff_dim), lambda i, s: (i, 0))] + specs,
            out_specs=pl.BlockSpec((rb, cols), lambda i, s: (i, 0)),
        ),
        out_shape=jax.ShapeDtypeStruct((rows, cols), jnp.bfloat16),
        compiler_params=pltpu.CompilerParams(dimension_semantics=("arbitrary",), vmem_limit_bytes=48 * 2**20),
        cost_estimate=pl.CostEstimate(flops=2 * rows * cols * ff_dim, bytes_accessed=2 * (rows * cols + cols * ff_dim + rows * ff_dim), transcendentals=0),
        name=name,
    )(ids, mid, *weights)


def combine_kernel(hid_ref, scale_ref, *refs):
    out_ref = refs[-1]
    half = out_ref.shape[1] // 2
    sides = [hid_ref[:, :half].astype(jnp.float32), hid_ref[:, half:].astype(jnp.float32)]
    mixed = [None, None]
    for k in range(len(refs) // 2):
        early, late = refs[2 * k], refs[2 * k + 1]
        rest = half - early.shape[1]
        own = jnp.concatenate([early[...], late[:, :rest]], axis=1).astype(jnp.float32)
        other = late[:, rest:].astype(jnp.float32)
        gate = scale_ref[:, 2 * k:2 * k + 1]
        flip = scale_ref[:, 2 * k + 1:2 * k + 2] > 0
        for side, value in enumerate((jnp.where(flip, other, own), jnp.where(flip, own, other))):
            term = value * gate
            mixed[side] = term if mixed[side] is None else mixed[side] + term
    out_ref[:, :half] = (sides[0] + mixed[0]).astype(out_ref.dtype)
    out_ref[:, half:] = (sides[1] + mixed[1]).astype(out_ref.dtype)


def combine(hidden, scale, parts):
    rows, model_dim = hidden.shape
    rb = 256
    return pl.pallas_call(
        combine_kernel,
        grid=(rows // rb,),
        in_specs=[pl.BlockSpec((rb, a.shape[1]), lambda i: (i, 0)) for a in (hidden, scale, *parts)],
        out_specs=pl.BlockSpec((rb, model_dim), lambda i: (i, 0)),
        out_shape=jax.ShapeDtypeStruct((rows, model_dim), jnp.bfloat16),
        compiler_params=pltpu.CompilerParams(dimension_semantics=("arbitrary",), vmem_limit_bytes=48 * 2**20),
        cost_estimate=pl.CostEstimate(flops=8 * rows * model_dim, bytes_accessed=8 * rows * model_dim, transcendentals=0),
        name="combine",
    )(hidden, scale, *parts)


def solution(mesh):
    tok_spec = P(('rep', 'expert', 'data'), None, None)
    group_axes = ('data', 'expert')
    token_axes = ('expert', 'data')
    data_size, expert_size = mesh.shape['data'], mesh.shape['expert']
    num_experts = expert_size * data_size
    other_data = [(0, 1), (1, 0)]
    other_chip = [(e, e ^ 2) for e in range(expert_size)]
    other_core = [(e, e ^ 1) for e in range(expert_size)]

    def local_step(x_loc, idx_loc, gate_loc, attn_gain, qkv_part, out_part, moe_gain, gate_part, up_part, down_part):
        num_seqs, seq_len, model_dim = x_loc.shape
        num_heads, head_dim = out_part.shape[0], out_part.shape[1]
        tok_dev = num_seqs * seq_len
        top_k = idx_loc.shape[-1]
        capacity = capacity_of(tok_dev, top_k, num_experts)
        half, ff_dim = gate_part.shape[1:]
        mine = lax.axis_index('data')
        place = lax.axis_index('expert')

        ids = jnp.stack([mine.astype(jnp.int32)])
        theirs = 1 - mine

        def plan(flat_ids):
            slot_pos = slots_of(flat_ids, num_experts)
            kept = slot_pos < capacity
            here = kept & (flat_ids % data_size == mine)
            slot = jnp.where(here, flat_ids // data_size * capacity + slot_pos, expert_size * capacity)
            source = jnp.zeros((expert_size * capacity,), jnp.int32)
            source = source.at[slot].set(jnp.arange(tok_dev * top_k, dtype=jnp.int32) // top_k, mode='drop')
            return kept, slot_pos, source

        flat_ids = idx_loc.reshape(tok_dev * top_k)
        kept, slot_pos, source = plan(flat_ids)
        _, _, peer_source = plan(lax.ppermute(flat_ids, 'data', other_data))

        def dispatch(normed, source):
            send = normed.at[source].get(mode='promise_in_bounds')
            return lax.all_to_all(send.reshape(expert_size, capacity, model_dim), 'expert', 0, 0, tiled=True).reshape(-1, model_dim)

        def spread(part, first):
            row = lax.dynamic_update_slice(jnp.zeros((data_size, expert_size) + part.shape, part.dtype), part[None, None], (mine, place, 0, 0))
            along, over, row, first = lax.optimization_barrier((lax.ppermute(part, 'data', other_data), lax.ppermute(part, 'expert', other_chip), row, first))
            whole = row
            for row, pieces in ((mine, [part, over]), (1 - mine, [along, lax.ppermute(along, 'expert', other_chip)])):
                for chip, piece in enumerate(pieces):
                    there = place ^ (2 * chip)
                    if piece is not part:
                        whole = lax.dynamic_update_slice(whole, piece[None, None], (row, there, 0, 0))
                    whole = lax.dynamic_update_slice(whole, lax.ppermute(piece, 'expert', other_core)[None, None], (row, there ^ 1, 0, 0))
            return whole.reshape(-1, part.shape[1]), first

        ff = tile_of(ff_dim, 384)
        split = (ff_dim // ff + 1) // 2 * ff
        sends = [lax.dynamic_slice(p, (theirs, 0, first), (1, half, size))[0] for first, size in ((0, split), (split, ff_dim - split)) for p in (gate_part, up_part)]
        normed_x = rms_scale(x_loc, attn_gain).reshape(tok_dev, model_dim)
        out_t = out_part.reshape(num_heads * head_dim, -1).T
        w_qkv, (sends, out_t, normed_x, source) = spread(qkv_part.reshape(qkv_part.shape[0], -1), (sends, out_t, normed_x, source))
        got = [lax.all_gather(part, 'data') for part in sends[:2]]

        out_t, w_qkv = lax.optimization_barrier((out_t, w_qkv))
        qkv = jnp.dot(normed_x, w_qkv, preferred_element_type=jnp.float32).astype(jnp.bfloat16)
        w_out_t, qkv = spread(out_t, qkv)
        attended = attention_core(qkv, num_seqs, num_heads, head_dim)
        attn_proj = lax.dot_general(attended, w_out_t, (((1,), (1,)), ((), ())), preferred_element_type=jnp.float32)
        hidden = (x_loc.reshape(tok_dev, model_dim).astype(jnp.float32) + attn_proj).astype(jnp.bfloat16)

        normed = rms_scale(hidden, moe_gain)
        peer_normed = lax.ppermute(normed, 'data', other_data)
        own_rows = dispatch(normed, source)
        later = (sends[2:], lax.dynamic_index_in_dim(down_part, theirs, 0, keepdims=False))
        later, peer_normed = lax.optimization_barrier((later, peer_normed))
        peer_rows = dispatch(peer_normed, peer_source)
        got = got + [lax.ppermute(part, 'data', other_data)[None] for part in later[0]]
        got_down = lax.ppermute(later[1], 'data', other_data)
        mid = None
        for first, wg_got, wu_got in ((0, got[0], got[1]), (split, got[2], got[3])):
            for rows, peer in ((own_rows, False), (peer_rows, True)):
                mid = expert_up(ids, rows, gate_part, wg_got, up_part, wu_got, mid, first, ff, capacity, peer)

        early = half // 256 * 256
        late = 2 * half - early
        once = pl.Buffered(buffer_count=1)
        spec_early = pl.BlockSpec((1, ff_dim, early), lambda i, s: (s[0], 0, 0), pipeline_mode=once)
        spec_rest = pl.BlockSpec((1, ff_dim, half - early), lambda i, s: (s[0], 0, early // (half - early)), pipeline_mode=once)
        spec_got = pl.BlockSpec((ff_dim, half), lambda i, s: (0, 0), pipeline_mode=once)

        def back(cols):
            return lax.all_to_all(cols.reshape(num_experts, capacity, -1), token_axes, 0, 0, tiled=True).reshape(num_experts * capacity, -1)

        outs = expert_down(ids, mid, [down_part], [spec_early], early, "expert_down_own")
        outs, got_down = lax.optimization_barrier((outs, got_down))
        pieces = [back(outs), back(expert_down(ids, mid, [down_part, got_down], [spec_rest, spec_got], late, "expert_down_got"))]

        pick = jnp.where(kept, flat_ids * capacity + slot_pos, 0).reshape(tok_dev, top_k)
        scale = jnp.where(kept, gate_loc.reshape(tok_dev * top_k), 0.0)
        odd = (flat_ids % data_size).astype(jnp.float32)
        scale = jnp.stack([scale, odd], axis=1).reshape(tok_dev, 2 * top_k)
        parts = [p.at[pick[:, k]].get(mode='promise_in_bounds') for k in range(top_k) for p in pieces]
        return combine(hidden, scale, parts).reshape(num_seqs, seq_len, model_dim)

    in_specs = (tok_spec, tok_spec, tok_spec, P(None), P(group_axes, None, None), P(None, None, group_axes), P(None), P('expert', 'data', None), P('expert', 'data', None), P('expert', None, 'data'))
    return jax.shard_map(local_step, mesh=mesh, in_specs=in_specs, out_specs=tok_spec, check_vma=False)
```

```python
import functools

import jax
import jax.numpy as jnp
from jax import lax
from jax.experimental import pallas as pl
from jax.experimental.pallas import tpu as pltpu
from jax.sharding import PartitionSpec as P


NORM_EPS = 1e-6
ROPE_BASE = 10000.0


def rms_scale(tok_rows, gain):
    rows_f32 = tok_rows.astype(jnp.float32)
    inv_rms = lax.rsqrt(jnp.mean(rows_f32 * rows_f32, axis=-1, keepdims=True) + NORM_EPS)
    return (rows_f32 * inv_rms * gain).astype(jnp.bfloat16)


def rope_tables(seq_len, head_dim, lanes):
    half_dim = head_dim // 2
    inv_freq = ROPE_BASE ** (-jnp.arange(half_dim, dtype=jnp.float32) * 2.0 / head_dim)
    angles = jnp.arange(seq_len, dtype=jnp.float32)[:, None] * inv_freq[None, :]
    cos_b, sin_b = jnp.cos(angles), jnp.sin(angles)
    times = lanes // head_dim
    return jnp.tile(jnp.concatenate([cos_b, cos_b], axis=1), (1, times)), jnp.tile(jnp.concatenate([-sin_b, sin_b], axis=1), (1, times))


def attention_kernel(head_dim, num_heads, qkv_ref, cos_ref, sin_ref, out_ref):
    seq_len = qkv_ref.shape[0]
    lanes = cos_ref.shape[1]
    per_block = lanes // head_dim
    width = num_heads * head_dim
    lane = lax.broadcasted_iota(jnp.int32, (seq_len, lanes), 1)
    low = lane % head_dim < head_dim // 2
    row_id = lax.broadcasted_iota(jnp.int32, (seq_len, seq_len), 0)
    causal = row_id >= lax.broadcasted_iota(jnp.int32, (seq_len, seq_len), 1)
    causal = jnp.concatenate([causal] * per_block, axis=0)
    cos_b, sin_b = cos_ref[...], sin_ref[...]

    def rope(vals):
        vals = vals.astype(jnp.float32)
        turned = jnp.where(low, pltpu.roll(vals, lanes - head_dim // 2, 1), pltpu.roll(vals, head_dim // 2, 1))
        return vals * cos_b + turned * sin_b

    for start in range(0, width, lanes):
        queries = rope(qkv_ref[:, start:start + lanes])
        keys = rope(qkv_ref[:, width + start:width + start + lanes]).astype(jnp.bfloat16)
        values = qkv_ref[:, 2 * width + start:2 * width + start + lanes]
        stacked = jnp.concatenate([jnp.where(lane // head_dim == h, queries, 0.0) for h in range(per_block)], axis=0).astype(jnp.bfloat16)
        scores = lax.dot_general(stacked, keys, (((1,), (1,)), ((), ())), preferred_element_type=jnp.float32) * (head_dim ** -0.5)
        scores = jnp.where(causal, scores, -1e30)
        weights = jnp.exp(scores - jnp.max(scores, axis=1, keepdims=True))
        probs = (weights / jnp.sum(weights, axis=1, keepdims=True)).astype(jnp.bfloat16)
        mixed = jnp.dot(probs, values, preferred_element_type=jnp.float32)
        out = mixed[:seq_len]
        for h in range(1, per_block):
            out = jnp.where(lane // head_dim == h, mixed[h * seq_len:(h + 1) * seq_len], out)
        out_ref[:, start:start + lanes] = out.astype(out_ref.dtype)


def attention_core(qkv, num_seqs, num_heads, head_dim):
    rows, width = qkv.shape
    seq_len = rows // num_seqs
    lanes = 128
    cos_b, sin_b = rope_tables(seq_len, head_dim, lanes)
    table = pl.BlockSpec((seq_len, lanes), lambda i: (0, 0))
    return pl.pallas_call(
        functools.partial(attention_kernel, head_dim, num_heads),
        grid=(num_seqs,),
        in_specs=[pl.BlockSpec((seq_len, width), lambda i: (i, 0)), table, table],
        out_specs=pl.BlockSpec((seq_len, width // 3), lambda i: (i, 0)),
        out_shape=jax.ShapeDtypeStruct((rows, width // 3), jnp.bfloat16),
        compiler_params=pltpu.CompilerParams(dimension_semantics=("arbitrary",), vmem_limit_bytes=32 * 2**20),
        cost_estimate=pl.CostEstimate(flops=40 * 10**9, bytes_accessed=8 * rows * width // 3, transcendentals=rows * seq_len * num_heads),
        name="attention_core",
    )(qkv, cos_b, sin_b)


def capacity_of(tok_dev, top_k, num_experts):
    return 8 * ((5 * top_k * tok_dev + 32 * num_experts - 1) // (32 * num_experts))


def slots_of(flat_ids, num_experts):
    onehot = (flat_ids[:, None] == jnp.arange(num_experts, dtype=jnp.int32)[None, :]).astype(jnp.int32)
    earlier = jnp.cumsum(onehot, axis=0) - onehot
    return jnp.sum(earlier * onehot, axis=1)


def tile_of(size, most):
    return max(t for t in range(128, most + 1, 128) if size % t == 0)


def up_kernel(ids_ref, z_a, z_b, wg_a, wg_b, wu_a, wu_b, *refs):
    mid_ref = refs[-1]
    ff = mid_ref.shape[1]
    w_a = jnp.concatenate([wg_a[0], wu_a[0]], axis=1)
    w_b = jnp.concatenate([wg_b[0], wu_b[0]], axis=1)
    w = jnp.concatenate([w_a, w_b], axis=0)
    rows = mid_ref.shape[0]
    start = pl.multiple_of(pl.program_id(1) * rows, rows)
    z = jnp.concatenate([z_a[pl.ds(start, rows), :], z_b[pl.ds(start, rows), :]], axis=1)
    acc = jnp.dot(z, w, preferred_element_type=jnp.float32)
    act_gate = acc[:, :ff]
    mid_ref[...] = (act_gate * jax.nn.sigmoid(act_gate) * acc[:, ff:]).astype(mid_ref.dtype)


def expert_up(ids, z, wg_own, wg_got, wu_own, wu_got, mid, first, ff, capacity, peer):
    rows, model_dim = z.shape
    half = model_dim // 2
    size, ff_dim = wg_got.shape[2], wg_own.shape[2]
    tiles, skip = size // ff, first // ff
    own = pl.BlockSpec((1, half, ff), lambda j, i, s: (s[0], 0, skip + j))
    got = pl.BlockSpec((1, half, ff), lambda j, i, s: (0 if wg_got.shape[0] == 1 else 1 - s[0], 0, j))
    once = pl.Buffered(buffer_count=1)
    given = [] if mid is None else [mid]
    return pl.pallas_call(
        up_kernel,
        grid_spec=pltpu.PrefetchScalarGridSpec(
            num_scalar_prefetch=1,
            grid=(tiles, rows // capacity),
            in_specs=[
                pl.BlockSpec((rows, half), lambda j, i, s: (0, s[0]), pipeline_mode=once),
                pl.BlockSpec((rows, half), lambda j, i, s: (0, 1 - s[0]), pipeline_mode=once),
                own, got, own, got,
            ] + [pl.BlockSpec(memory_space=pl.ANY)] * len(given),
            out_specs=pl.BlockSpec((capacity, ff), lambda j, i, s: (2 * i + (1 - s[0] if peer else s[0]), skip + j)),
        ),
        out_shape=jax.ShapeDtypeStruct((2 * rows, ff_dim), jnp.bfloat16),
        input_output_aliases={7: 0} if given else {},
        compiler_params=pltpu.CompilerParams(dimension_semantics=("arbitrary", "arbitrary"), vmem_limit_bytes=48 * 2**20),
        cost_estimate=pl.CostEstimate(flops=4 * rows * model_dim * size, bytes_accessed=2 * (rows * model_dim + 2 * model_dim * size + rows * size), transcendentals=rows * size),
        name="expert_up",
    )(ids, z, z, wg_own, wg_got, wu_own, wu_got, *given)


def down_kernel(ids_ref, mid_ref, *refs):
    out_ref = refs[-1]
    w = [r[0] if len(r.shape) == 3 else r[...] for r in refs[:-1]]
    w = w[0] if len(w) == 1 else jnp.concatenate(w, axis=1)
    out_ref[...] = jnp.dot(mid_ref[...], w, preferred_element_type=jnp.float32).astype(out_ref.dtype)


def expert_down(ids, mid, weights, specs, cols):
    rows, ff_dim = mid.shape
    rb = tile_of(rows, 512)
    return pl.pallas_call(
        down_kernel,
        grid_spec=pltpu.PrefetchScalarGridSpec(
            num_scalar_prefetch=1,
            grid=(rows // rb,),
            in_specs=[pl.BlockSpec((rb, ff_dim), lambda i, s: (i, 0))] + specs,
            out_specs=pl.BlockSpec((rb, cols), lambda i, s: (i, 0)),
        ),
        out_shape=jax.ShapeDtypeStruct((rows, cols), jnp.bfloat16),
        compiler_params=pltpu.CompilerParams(dimension_semantics=("arbitrary",), vmem_limit_bytes=48 * 2**20),
        cost_estimate=pl.CostEstimate(flops=2 * rows * cols * ff_dim, bytes_accessed=2 * (rows * cols + cols * ff_dim + rows * ff_dim), transcendentals=0),
    )(ids, mid, *weights)


def combine_kernel(hid_ref, scale_ref, *refs):
    out_ref = refs[-1]
    half = out_ref.shape[1] // 2
    sides = [hid_ref[:, :half].astype(jnp.float32), hid_ref[:, half:].astype(jnp.float32)]
    mixed = [None, None]
    for k in range(len(refs) // 2):
        early, late = refs[2 * k], refs[2 * k + 1]
        rest = half - early.shape[1]
        own = jnp.concatenate([early[...], late[:, :rest]], axis=1).astype(jnp.float32)
        other = late[:, rest:].astype(jnp.float32)
        gate = scale_ref[:, 2 * k:2 * k + 1]
        flip = scale_ref[:, 2 * k + 1:2 * k + 2] > 0
        for side, value in enumerate((jnp.where(flip, other, own), jnp.where(flip, own, other))):
            term = value * gate
            mixed[side] = term if mixed[side] is None else mixed[side] + term
    out_ref[:, :half] = (sides[0] + mixed[0]).astype(out_ref.dtype)
    out_ref[:, half:] = (sides[1] + mixed[1]).astype(out_ref.dtype)


def combine(hidden, scale, parts):
    rows, model_dim = hidden.shape
    rb = 256
    return pl.pallas_call(
        combine_kernel,
        grid=(rows // rb,),
        in_specs=[pl.BlockSpec((rb, a.shape[1]), lambda i: (i, 0)) for a in (hidden, scale, *parts)],
        out_specs=pl.BlockSpec((rb, model_dim), lambda i: (i, 0)),
        out_shape=jax.ShapeDtypeStruct((rows, model_dim), jnp.bfloat16),
        compiler_params=pltpu.CompilerParams(dimension_semantics=("arbitrary",), vmem_limit_bytes=48 * 2**20),
        cost_estimate=pl.CostEstimate(flops=8 * rows * model_dim, bytes_accessed=8 * rows * model_dim, transcendentals=0),
        name="combine",
    )(hidden, scale, *parts)


def solution(mesh):
    tok_spec = P(('rep', 'expert', 'data'), None, None)
    group_axes = ('data', 'expert')
    token_axes = ('expert', 'data')
    data_size, expert_size = mesh.shape['data'], mesh.shape['expert']
    num_experts = expert_size * data_size
    other_data = [(0, 1), (1, 0)]
    other_chip = [(e, e ^ 2) for e in range(expert_size)]
    other_core = [(e, e ^ 1) for e in range(expert_size)]

    def local_step(x_loc, idx_loc, gate_loc, attn_gain, qkv_part, out_part, moe_gain, gate_part, up_part, down_part):
        num_seqs, seq_len, model_dim = x_loc.shape
        num_heads, head_dim = out_part.shape[0], out_part.shape[1]
        tok_dev = num_seqs * seq_len
        top_k = idx_loc.shape[-1]
        capacity = capacity_of(tok_dev, top_k, num_experts)
        half, ff_dim = gate_part.shape[1:]
        mine = lax.axis_index('data')
        place = lax.axis_index('expert')

        ids = jnp.stack([mine.astype(jnp.int32)])
        theirs = 1 - mine

        def swap(value):
            return lax.ppermute(value, 'data', other_data)

        def cross(value):
            return lax.ppermute(value, 'expert', other_chip)

        def plan(flat_ids):
            slot_pos = slots_of(flat_ids, num_experts)
            kept = slot_pos < capacity
            here = kept & (flat_ids % data_size == mine)
            slot = jnp.where(here, flat_ids // data_size * capacity + slot_pos, expert_size * capacity)
            source = jnp.zeros((expert_size * capacity,), jnp.int32)
            source = source.at[slot].set(jnp.arange(tok_dev * top_k, dtype=jnp.int32) // top_k, mode='drop')
            return kept, slot_pos, source

        flat_ids = idx_loc.reshape(tok_dev * top_k)
        kept, slot_pos, source = plan(flat_ids)
        _, _, peer_source = plan(swap(flat_ids))

        def dispatch(normed, source):
            send = normed.at[source].get(mode='promise_in_bounds')
            return lax.all_to_all(send.reshape(expert_size, capacity, model_dim), 'expert', 0, 0, tiled=True).reshape(-1, model_dim)

        def spread(part, first):
            row = lax.dynamic_update_slice(jnp.zeros((data_size, expert_size) + part.shape, part.dtype), part[None, None], (mine, place, 0, 0))
            along, over, row, first = lax.optimization_barrier((swap(part), cross(part), row, first))
            whole = row
            for row, pieces in ((mine, [part, over]), (1 - mine, [along, cross(along)])):
                for chip, piece in enumerate(pieces):
                    there = place ^ (2 * chip)
                    if piece is not part:
                        whole = lax.dynamic_update_slice(whole, piece[None, None], (row, there, 0, 0))
                    whole = lax.dynamic_update_slice(whole, lax.ppermute(piece, 'expert', other_core)[None, None], (row, there ^ 1, 0, 0))
            return whole.reshape(-1, part.shape[1]), first

        ff = tile_of(ff_dim, 384)
        split = (ff_dim // ff + 1) // 2 * ff
        sends = [lax.dynamic_slice(p, (theirs, 0, first), (1, half, size))[0] for first, size in ((0, split), (split, ff_dim - split)) for p in (gate_part, up_part)]
        normed_x = rms_scale(x_loc, attn_gain).reshape(tok_dev, model_dim)
        out_t = out_part.reshape(num_heads * head_dim, -1).T
        w_qkv, (normed_x, source) = spread(qkv_part.reshape(qkv_part.shape[0], -1), (normed_x, source))
        got = [swap(part)[None] for part in sends]
        got_down = swap(lax.dynamic_index_in_dim(down_part, theirs, 0, keepdims=False))

        qkv = jnp.dot(normed_x, w_qkv, preferred_element_type=jnp.float32).astype(jnp.bfloat16)
        w_out_t, qkv = spread(out_t, qkv)
        attended = attention_core(qkv, num_seqs, num_heads, head_dim)
        attn_proj = lax.dot_general(attended, w_out_t, (((1,), (1,)), ((), ())), preferred_element_type=jnp.float32)
        hidden = (x_loc.reshape(tok_dev, model_dim).astype(jnp.float32) + attn_proj).astype(jnp.bfloat16)

        normed = rms_scale(hidden, moe_gain)
        peer_normed = swap(normed)
        own_rows = dispatch(normed, source)
        peer_rows = dispatch(peer_normed, peer_source)
        mid = None
        for first, wg_got, wu_got in ((0, got[0], got[1]), (split, got[2], got[3])):
            for rows, peer in ((own_rows, False), (peer_rows, True)):
                mid = expert_up(ids, rows, gate_part, wg_got, up_part, wu_got, mid, first, ff, capacity, peer)

        early = half // 256 * 256
        late = 2 * half - early
        once = pl.Buffered(buffer_count=1)
        spec_early = pl.BlockSpec((1, ff_dim, early), lambda i, s: (s[0], 0, 0), pipeline_mode=once)
        spec_rest = pl.BlockSpec((1, ff_dim, half - early), lambda i, s: (s[0], 0, early // (half - early)), pipeline_mode=once)
        spec_got = pl.BlockSpec((ff_dim, half), lambda i, s: (0, 0), pipeline_mode=once)

        def back(cols):
            return lax.all_to_all(cols.reshape(num_experts, capacity, -1), token_axes, 0, 0, tiled=True).reshape(num_experts * capacity, -1)

        outs = expert_down(ids, mid, [down_part], [spec_early], early)
        outs, got_down = lax.optimization_barrier((outs, got_down))
        pieces = [back(outs), back(expert_down(ids, mid, [down_part, got_down], [spec_rest, spec_got], late))]

        pick = jnp.where(kept, flat_ids * capacity + slot_pos, 0).reshape(tok_dev, top_k)
        scale = jnp.where(kept, gate_loc.reshape(tok_dev * top_k), 0.0)
        odd = (flat_ids % data_size).astype(jnp.float32)
        scale = jnp.stack([scale, odd], axis=1).reshape(tok_dev, 2 * top_k)
        parts = [p.at[pick[:, k]].get(mode='promise_in_bounds') for k in range(top_k) for p in pieces]
        return combine(hidden, scale, parts).reshape(num_seqs, seq_len, model_dim)

    in_specs = (tok_spec, tok_spec, tok_spec, P(None), P(group_axes, None, None), P(None, None, group_axes), P(None), P('expert', 'data', None), P('expert', 'data', None), P('expert', None, 'data'))

    return jax.shard_map(local_step, mesh=mesh, in_specs=in_specs, out_specs=tok_spec, check_vma=False)
```

```python
import functools

import jax
import jax.numpy as jnp
from jax import lax
from jax.experimental import pallas as pl
from jax.experimental.pallas import tpu as pltpu
from jax.sharding import PartitionSpec as P


NORM_EPS = 1e-6
ROPE_BASE = 10000.0


def rms_scale(tok_rows, gain):
    rows_f32 = tok_rows.astype(jnp.float32)
    inv_rms = lax.rsqrt(jnp.mean(rows_f32 * rows_f32, axis=-1, keepdims=True) + NORM_EPS)
    return (rows_f32 * inv_rms * gain).astype(jnp.bfloat16)


def rope_tables(seq_len, head_dim, lanes):
    half_dim = head_dim // 2
    inv_freq = ROPE_BASE ** (-jnp.arange(half_dim, dtype=jnp.float32) * 2.0 / head_dim)
    angles = jnp.arange(seq_len, dtype=jnp.float32)[:, None] * inv_freq[None, :]
    cos_b, sin_b = jnp.cos(angles), jnp.sin(angles)
    times = lanes // head_dim
    return jnp.tile(jnp.concatenate([cos_b, cos_b], axis=1), (1, times)), jnp.tile(jnp.concatenate([-sin_b, sin_b], axis=1), (1, times))


def attention_kernel(head_dim, num_heads, qkv_ref, cos_ref, sin_ref, out_ref):
    seq_len = qkv_ref.shape[0]
    lanes = cos_ref.shape[1]
    per_block = lanes // head_dim
    width = num_heads * head_dim
    lane = lax.broadcasted_iota(jnp.int32, (seq_len, lanes), 1)
    low = lane % head_dim < head_dim // 2
    row_id = lax.broadcasted_iota(jnp.int32, (seq_len, seq_len), 0)
    causal = row_id >= lax.broadcasted_iota(jnp.int32, (seq_len, seq_len), 1)
    causal = jnp.concatenate([causal] * per_block, axis=0)
    cos_b, sin_b = cos_ref[...], sin_ref[...]

    def rope(vals):
        vals = vals.astype(jnp.float32)
        turned = jnp.where(low, pltpu.roll(vals, lanes - head_dim // 2, 1), pltpu.roll(vals, head_dim // 2, 1))
        return vals * cos_b + turned * sin_b

    for start in range(0, width, lanes):
        queries = rope(qkv_ref[:, start:start + lanes])
        keys = rope(qkv_ref[:, width + start:width + start + lanes]).astype(jnp.bfloat16)
        values = qkv_ref[:, 2 * width + start:2 * width + start + lanes]
        stacked = jnp.concatenate([jnp.where(lane // head_dim == h, queries, 0.0) for h in range(per_block)], axis=0).astype(jnp.bfloat16)
        scores = lax.dot_general(stacked, keys, (((1,), (1,)), ((), ())), preferred_element_type=jnp.float32) * (head_dim ** -0.5)
        scores = jnp.where(causal, scores, -1e30)
        weights = jnp.exp(scores - jnp.max(scores, axis=1, keepdims=True))
        probs = (weights / jnp.sum(weights, axis=1, keepdims=True)).astype(jnp.bfloat16)
        mixed = jnp.dot(probs, values, preferred_element_type=jnp.float32)
        out = mixed[:seq_len]
        for h in range(1, per_block):
            out = jnp.where(lane // head_dim == h, mixed[h * seq_len:(h + 1) * seq_len], out)
        out_ref[:, start:start + lanes] = out.astype(out_ref.dtype)


def attention_core(qkv, num_seqs, num_heads, head_dim):
    rows, width = qkv.shape
    seq_len = rows // num_seqs
    lanes = 128
    cos_b, sin_b = rope_tables(seq_len, head_dim, lanes)
    table = pl.BlockSpec((seq_len, lanes), lambda i: (0, 0))
    return pl.pallas_call(
        functools.partial(attention_kernel, head_dim, num_heads),
        grid=(num_seqs,),
        in_specs=[pl.BlockSpec((seq_len, width), lambda i: (i, 0)), table, table],
        out_specs=pl.BlockSpec((seq_len, width // 3), lambda i: (i, 0)),
        out_shape=jax.ShapeDtypeStruct((rows, width // 3), jnp.bfloat16),
        compiler_params=pltpu.CompilerParams(dimension_semantics=("arbitrary",), vmem_limit_bytes=32 * 2**20),
        cost_estimate=pl.CostEstimate(flops=40 * 10**9, bytes_accessed=8 * rows * width // 3, transcendentals=rows * seq_len * num_heads),
        name="attention_core",
    )(qkv, cos_b, sin_b)


def capacity_of(tok_dev, top_k, num_experts):
    return 8 * ((5 * top_k * tok_dev + 32 * num_experts - 1) // (32 * num_experts))


def slots_of(flat_ids, num_experts):
    onehot = (flat_ids[:, None] == jnp.arange(num_experts, dtype=jnp.int32)[None, :]).astype(jnp.int32)
    earlier = jnp.cumsum(onehot, axis=0) - onehot
    return jnp.sum(earlier * onehot, axis=1)


def tile_of(size, most):
    return max(t for t in range(128, most + 1, 128) if size % t == 0)


def up_kernel(ids_ref, z_a, z_b, wg_a, wg_b, wu_a, wu_b, *refs):
    mid_ref = refs[-1]
    ff = mid_ref.shape[1]
    w_a = jnp.concatenate([wg_a[0], wu_a[0]], axis=1)
    w_b = jnp.concatenate([wg_b[0], wu_b[0]], axis=1)
    w = jnp.concatenate([w_a, w_b], axis=0)
    rows = mid_ref.shape[0]
    start = pl.multiple_of(pl.program_id(1) * rows, rows)
    z = jnp.concatenate([z_a[pl.ds(start, rows), :], z_b[pl.ds(start, rows), :]], axis=1)
    acc = jnp.dot(z, w, preferred_element_type=jnp.float32)
    act_gate = acc[:, :ff]
    mid_ref[...] = (act_gate * jax.nn.sigmoid(act_gate) * acc[:, ff:]).astype(mid_ref.dtype)


def expert_up(ids, z, wg_own, wg_got, wu_own, wu_got, mid, first, ff, capacity, peer):
    rows, model_dim = z.shape
    half = model_dim // 2
    size, ff_dim = wg_got.shape[2], wg_own.shape[2]
    tiles, skip = size // ff, first // ff
    own = pl.BlockSpec((1, half, ff), lambda j, i, s: (s[0], 0, skip + j))
    got = pl.BlockSpec((1, half, ff), lambda j, i, s: (0 if wg_got.shape[0] == 1 else 1 - s[0], 0, j))
    once = pl.Buffered(buffer_count=1)
    given = [] if mid is None else [mid]
    return pl.pallas_call(
        up_kernel,
        grid_spec=pltpu.PrefetchScalarGridSpec(
            num_scalar_prefetch=1,
            grid=(tiles, rows // capacity),
            in_specs=[
                pl.BlockSpec((rows, half), lambda j, i, s: (0, s[0]), pipeline_mode=once),
                pl.BlockSpec((rows, half), lambda j, i, s: (0, 1 - s[0]), pipeline_mode=once),
                own, got, own, got,
            ] + [pl.BlockSpec(memory_space=pl.ANY)] * len(given),
            out_specs=pl.BlockSpec((capacity, ff), lambda j, i, s: (2 * i + (1 - s[0] if peer else s[0]), skip + j)),
        ),
        out_shape=jax.ShapeDtypeStruct((2 * rows, ff_dim), jnp.bfloat16),
        input_output_aliases={7: 0} if given else {},
        compiler_params=pltpu.CompilerParams(dimension_semantics=("arbitrary", "arbitrary"), vmem_limit_bytes=48 * 2**20),
        cost_estimate=pl.CostEstimate(flops=4 * rows * model_dim * size, bytes_accessed=2 * (rows * model_dim + 2 * model_dim * size + rows * size), transcendentals=rows * size),
        name="expert_up",
    )(ids, z, z, wg_own, wg_got, wu_own, wu_got, *given)


def down_kernel(ids_ref, mid_ref, *refs):
    out_ref = refs[-1]
    w = [r[0] if len(r.shape) == 3 else r[...] for r in refs[:-1]]
    w = w[0] if len(w) == 1 else jnp.concatenate(w, axis=1)
    out_ref[...] = jnp.dot(mid_ref[...], w, preferred_element_type=jnp.float32).astype(out_ref.dtype)


def expert_down(ids, mid, weights, specs, cols):
    rows, ff_dim = mid.shape
    rb = tile_of(rows, 512)
    return pl.pallas_call(
        down_kernel,
        grid_spec=pltpu.PrefetchScalarGridSpec(
            num_scalar_prefetch=1,
            grid=(rows // rb,),
            in_specs=[pl.BlockSpec((rb, ff_dim), lambda i, s: (i, 0))] + specs,
            out_specs=pl.BlockSpec((rb, cols), lambda i, s: (i, 0)),
        ),
        out_shape=jax.ShapeDtypeStruct((rows, cols), jnp.bfloat16),
        compiler_params=pltpu.CompilerParams(dimension_semantics=("arbitrary",), vmem_limit_bytes=48 * 2**20),
        cost_estimate=pl.CostEstimate(flops=2 * rows * cols * ff_dim, bytes_accessed=2 * (rows * cols + cols * ff_dim + rows * ff_dim), transcendentals=0),
    )(ids, mid, *weights)


def combine_kernel(hid_ref, scale_ref, *refs):
    out_ref = refs[-1]
    half = out_ref.shape[1] // 2
    sides = [hid_ref[:, :half].astype(jnp.float32), hid_ref[:, half:].astype(jnp.float32)]
    mixed = [None, None]
    for k in range(len(refs) // 2):
        early, late = refs[2 * k], refs[2 * k + 1]
        own = early[:, :half].astype(jnp.float32)
        other = jnp.concatenate([early[:, half:], late[...]], axis=1).astype(jnp.float32)
        gate = scale_ref[:, 2 * k:2 * k + 1]
        flip = scale_ref[:, 2 * k + 1:2 * k + 2] > 0
        for side, value in enumerate((jnp.where(flip, other, own), jnp.where(flip, own, other))):
            term = value * gate
            mixed[side] = term if mixed[side] is None else mixed[side] + term
    out_ref[:, :half] = (sides[0] + mixed[0]).astype(out_ref.dtype)
    out_ref[:, half:] = (sides[1] + mixed[1]).astype(out_ref.dtype)


def combine(hidden, scale, parts):
    rows, model_dim = hidden.shape
    rb = 256
    return pl.pallas_call(
        combine_kernel,
        grid=(rows // rb,),
        in_specs=[pl.BlockSpec((rb, a.shape[1]), lambda i: (i, 0)) for a in (hidden, scale, *parts)],
        out_specs=pl.BlockSpec((rb, model_dim), lambda i: (i, 0)),
        out_shape=jax.ShapeDtypeStruct((rows, model_dim), jnp.bfloat16),
        compiler_params=pltpu.CompilerParams(dimension_semantics=("arbitrary",), vmem_limit_bytes=48 * 2**20),
        cost_estimate=pl.CostEstimate(flops=8 * rows * model_dim, bytes_accessed=8 * rows * model_dim, transcendentals=0),
        name="combine",
    )(hidden, scale, *parts)


def solution(mesh):
    tok_spec = P(('rep', 'expert', 'data'), None, None)
    group_axes = ('data', 'expert')
    token_axes = ('expert', 'data')
    data_size, expert_size = mesh.shape['data'], mesh.shape['expert']
    num_experts = expert_size * data_size
    other_data = [(0, 1), (1, 0)]
    other_chip = [(e, e ^ 2) for e in range(expert_size)]
    other_core = [(e, e ^ 1) for e in range(expert_size)]

    def local_step(x_loc, idx_loc, gate_loc, attn_gain, qkv_part, out_part, moe_gain, gate_part, up_part, down_part):
        num_seqs, seq_len, model_dim = x_loc.shape
        num_heads, head_dim = out_part.shape[0], out_part.shape[1]
        tok_dev = num_seqs * seq_len
        top_k = idx_loc.shape[-1]
        capacity = capacity_of(tok_dev, top_k, num_experts)
        half, ff_dim = gate_part.shape[1:]
        mine = lax.axis_index('data')
        place = lax.axis_index('expert')

        ids = jnp.stack([mine.astype(jnp.int32)])
        theirs = 1 - mine

        def swap(value):
            return lax.ppermute(value, 'data', other_data)

        def cross(value):
            return lax.ppermute(value, 'expert', other_chip)

        def plan(flat_ids):
            slot_pos = slots_of(flat_ids, num_experts)
            kept = slot_pos < capacity
            here = kept & (flat_ids % data_size == mine)
            slot = jnp.where(here, flat_ids // data_size * capacity + slot_pos, expert_size * capacity)
            source = jnp.zeros((expert_size * capacity,), jnp.int32)
            source = source.at[slot].set(jnp.arange(tok_dev * top_k, dtype=jnp.int32) // top_k, mode='drop')
            return kept, slot_pos, source

        flat_ids = idx_loc.reshape(tok_dev * top_k)
        kept, slot_pos, source = plan(flat_ids)
        _, _, peer_source = plan(swap(flat_ids))

        def dispatch(normed, source):
            send = normed.at[source].get(mode='promise_in_bounds')
            return lax.all_to_all(send.reshape(expert_size, capacity, model_dim), 'expert', 0, 0, tiled=True).reshape(-1, model_dim)

        def spread(part, first):
            row = lax.dynamic_update_slice(jnp.zeros((data_size, expert_size) + part.shape, part.dtype), part[None, None], (mine, place, 0, 0))
            along, over, row, first = lax.optimization_barrier((swap(part), cross(part), row, first))
            whole = row
            for row, pieces in ((mine, [part, over]), (1 - mine, [along, cross(along)])):
                for chip, piece in enumerate(pieces):
                    there = place ^ (2 * chip)
                    if piece is not part:
                        whole = lax.dynamic_update_slice(whole, piece[None, None], (row, there, 0, 0))
                    whole = lax.dynamic_update_slice(whole, lax.ppermute(piece, 'expert', other_core)[None, None], (row, there ^ 1, 0, 0))
            return whole.reshape(-1, part.shape[1]), first

        ff = tile_of(ff_dim, 384)
        split = (ff_dim // ff + 1) // 2 * ff
        sends = [lax.dynamic_slice(p, (theirs, 0, first), (1, half, size))[0] for first, size in ((0, split), (split, ff_dim - split)) for p in (gate_part, up_part)]
        normed_x = rms_scale(x_loc, attn_gain).reshape(tok_dev, model_dim)
        out_t = out_part.reshape(num_heads * head_dim, -1).T
        qkv_part, out_t = lax.optimization_barrier((qkv_part, out_t))
        qkv_flat = qkv_part.reshape(qkv_part.shape[0], -1)
        w_qkv, (normed_x, source) = spread(qkv_flat, (normed_x, source))
        got = [swap(part)[None] for part in sends]
        more = half - half // 2 // 256 * 256
        got_down = [swap(lax.dynamic_slice(down_part, (theirs, 0, first), (1, ff_dim, size))[0]) for first, size in ((0, more), (more, half - more))]

        qkv = jnp.dot(normed_x, w_qkv, preferred_element_type=jnp.float32).astype(jnp.bfloat16)
        w_out_t, qkv = spread(out_t, qkv)
        attended = attention_core(qkv, num_seqs, num_heads, head_dim)
        attn_proj = lax.dot_general(attended, w_out_t, (((1,), (1,)), ((), ())), preferred_element_type=jnp.float32)
        hidden = (x_loc.reshape(tok_dev, model_dim).astype(jnp.float32) + attn_proj).astype(jnp.bfloat16)

        normed = rms_scale(hidden, moe_gain)
        peer_normed = swap(normed)
        own_rows = dispatch(normed, source)
        peer_rows = dispatch(peer_normed, peer_source)
        mid = None
        for first, wg_got, wu_got in ((0, got[0], got[1]), (split, got[2], got[3])):
            for rows, peer in ((own_rows, False), (peer_rows, True)):
                mid = expert_up(ids, rows, gate_part, wg_got, up_part, wu_got, mid, first, ff, capacity, peer)

        once = pl.Buffered(buffer_count=1)
        spec_own = pl.BlockSpec((1, ff_dim, half), lambda i, s: (s[0], 0, 0), pipeline_mode=once)
        spec_got = [pl.BlockSpec(part.shape, lambda i, s: (0, 0), pipeline_mode=once) for part in got_down]

        def back(cols):
            return lax.all_to_all(cols.reshape(num_experts, capacity, -1), token_axes, 0, 0, tiled=True).reshape(num_experts * capacity, -1)

        outs = expert_down(ids, mid, [down_part, got_down[0]], [spec_own, spec_got[0]], half + more)
        outs, last_down = lax.optimization_barrier((outs, got_down[1]))
        last_outs = expert_down(ids, mid, [last_down], [spec_got[1]], half - more)
        pieces = [back(outs), back(last_outs)]

        pick = jnp.where(kept, flat_ids * capacity + slot_pos, 0).reshape(tok_dev, top_k)
        scale = jnp.where(kept, gate_loc.reshape(tok_dev * top_k), 0.0)
        odd = (flat_ids % data_size).astype(jnp.float32)
        scale = jnp.stack([scale, odd], axis=1).reshape(tok_dev, 2 * top_k)
        parts = [p.at[pick[:, k]].get(mode='promise_in_bounds') for k in range(top_k) for p in pieces]
        return combine(hidden, scale, parts).reshape(num_seqs, seq_len, model_dim)

    in_specs = (tok_spec, tok_spec, tok_spec, P(None), P(group_axes, None, None), P(None, None, group_axes), P(None), P('expert', 'data', None), P('expert', 'data', None), P('expert', None, 'data'))

    return jax.shard_map(local_step, mesh=mesh, in_specs=in_specs, out_specs=tok_spec, check_vma=False)
```

```python
import functools

import jax
import jax.numpy as jnp
from jax import lax
from jax.experimental import pallas as pl
from jax.experimental.pallas import tpu as pltpu
from jax.sharding import PartitionSpec as P


NORM_EPS = 1e-6
ROPE_BASE = 10000.0


def rms_scale(tok_rows, gain):
    rows_f32 = tok_rows.astype(jnp.float32)
    inv_rms = lax.rsqrt(jnp.mean(rows_f32 * rows_f32, axis=-1, keepdims=True) + NORM_EPS)
    return (rows_f32 * inv_rms * gain).astype(jnp.bfloat16)


def rope_tables(seq_len, head_dim, lanes):
    half_dim = head_dim // 2
    inv_freq = ROPE_BASE ** (-jnp.arange(half_dim, dtype=jnp.float32) * 2.0 / head_dim)
    angles = jnp.arange(seq_len, dtype=jnp.float32)[:, None] * inv_freq[None, :]
    cos_b, sin_b = jnp.cos(angles), jnp.sin(angles)
    times = lanes // head_dim
    return jnp.tile(jnp.concatenate([cos_b, cos_b], axis=1), (1, times)), jnp.tile(jnp.concatenate([-sin_b, sin_b], axis=1), (1, times))


def attention_kernel(head_dim, num_heads, qkv_ref, cos_ref, sin_ref, out_ref):
    seq_len = qkv_ref.shape[0]
    lanes = cos_ref.shape[1]
    per_block = lanes // head_dim
    width = num_heads * head_dim
    lane = lax.broadcasted_iota(jnp.int32, (seq_len, lanes), 1)
    low = lane % head_dim < head_dim // 2
    row_id = lax.broadcasted_iota(jnp.int32, (seq_len, seq_len), 0)
    causal = row_id >= lax.broadcasted_iota(jnp.int32, (seq_len, seq_len), 1)
    causal = jnp.concatenate([causal] * per_block, axis=0)
    cos_b, sin_b = cos_ref[...], sin_ref[...]

    def rope(vals):
        vals = vals.astype(jnp.float32)
        turned = jnp.where(low, pltpu.roll(vals, lanes - head_dim // 2, 1), pltpu.roll(vals, head_dim // 2, 1))
        return vals * cos_b + turned * sin_b

    for start in range(0, width, lanes):
        queries = rope(qkv_ref[:, start:start + lanes])
        keys = rope(qkv_ref[:, width + start:width + start + lanes]).astype(jnp.bfloat16)
        values = qkv_ref[:, 2 * width + start:2 * width + start + lanes]
        stacked = jnp.concatenate([jnp.where(lane // head_dim == h, queries, 0.0) for h in range(per_block)], axis=0).astype(jnp.bfloat16)
        scores = lax.dot_general(stacked, keys, (((1,), (1,)), ((), ())), preferred_element_type=jnp.float32) * (head_dim ** -0.5)
        scores = jnp.where(causal, scores, -1e30)
        weights = jnp.exp(scores - jnp.max(scores, axis=1, keepdims=True))
        probs = (weights / jnp.sum(weights, axis=1, keepdims=True)).astype(jnp.bfloat16)
        mixed = jnp.dot(probs, values, preferred_element_type=jnp.float32)
        out = mixed[:seq_len]
        for h in range(1, per_block):
            out = jnp.where(lane // head_dim == h, mixed[h * seq_len:(h + 1) * seq_len], out)
        out_ref[:, start:start + lanes] = out.astype(out_ref.dtype)


def attention_core(qkv, num_seqs, num_heads, head_dim):
    rows, width = qkv.shape
    seq_len = rows // num_seqs
    lanes = 128
    cos_b, sin_b = rope_tables(seq_len, head_dim, lanes)
    table = pl.BlockSpec((seq_len, lanes), lambda i: (0, 0))
    return pl.pallas_call(
        functools.partial(attention_kernel, head_dim, num_heads),
        grid=(num_seqs,),
        in_specs=[pl.BlockSpec((seq_len, width), lambda i: (i, 0)), table, table],
        out_specs=pl.BlockSpec((seq_len, width // 3), lambda i: (i, 0)),
        out_shape=jax.ShapeDtypeStruct((rows, width // 3), jnp.bfloat16),
        compiler_params=pltpu.CompilerParams(dimension_semantics=("arbitrary",), vmem_limit_bytes=32 * 2**20),
        cost_estimate=pl.CostEstimate(flops=40 * 10**9, bytes_accessed=8 * rows * width // 3, transcendentals=rows * seq_len * num_heads),
        name="attention_core",
    )(qkv, cos_b, sin_b)


def capacity_of(tok_dev, top_k, num_experts):
    return 8 * ((5 * top_k * tok_dev + 32 * num_experts - 1) // (32 * num_experts))


def slots_of(flat_ids, num_experts):
    onehot = (flat_ids[:, None] == jnp.arange(num_experts, dtype=jnp.int32)[None, :]).astype(jnp.int32)
    earlier = jnp.cumsum(onehot, axis=0) - onehot
    return jnp.sum(earlier * onehot, axis=1)


def tile_of(size, most):
    return max(t for t in range(128, most + 1, 128) if size % t == 0)


def up_kernel(ids_ref, z_a, z_b, wg_a, wg_b, wu_a, wu_b, *refs):
    mid_ref = refs[-1]
    ff = mid_ref.shape[2]
    w_a = jnp.concatenate([wg_a[0], wu_a[0]], axis=1)
    w_b = jnp.concatenate([wg_b[0], wu_b[0]], axis=1)
    w = jnp.concatenate([w_a, w_b], axis=0)
    rows = mid_ref.shape[0] * mid_ref.shape[1]
    start = pl.multiple_of(pl.program_id(1) * rows, rows)
    z = jnp.concatenate([z_a[pl.ds(start, rows), :], z_b[pl.ds(start, rows), :]], axis=1)
    acc = jnp.dot(z, w, preferred_element_type=jnp.float32)
    act_gate = acc[:, :ff]
    mid_ref[...] = (act_gate * jax.nn.sigmoid(act_gate) * acc[:, ff:]).astype(mid_ref.dtype).reshape(mid_ref.shape)


def expert_up(ids, z, wg_own, wg_got, wu_own, wu_got, mid, first, ff, capacity, peer):
    rows, model_dim = z.shape
    half = model_dim // 2
    size, ff_dim = wg_got.shape[2], wg_own.shape[2]
    tiles, skip = size // ff, first // ff
    devices = rows // capacity
    pair = 2 if devices % 2 == 0 else 1
    own = pl.BlockSpec((1, half, ff), lambda j, i, s: (s[0], 0, skip + j))
    got = pl.BlockSpec((1, half, ff), lambda j, i, s: (0 if wg_got.shape[0] == 1 else 1 - s[0], 0, j))
    once = pl.Buffered(buffer_count=1)
    given = [] if mid is None else [mid]
    return pl.pallas_call(
        up_kernel,
        grid_spec=pltpu.PrefetchScalarGridSpec(
            num_scalar_prefetch=1,
            grid=(tiles, devices // pair),
            in_specs=[
                pl.BlockSpec((rows, half), lambda j, i, s: (0, s[0]), pipeline_mode=once),
                pl.BlockSpec((rows, half), lambda j, i, s: (0, 1 - s[0]), pipeline_mode=once),
                own, got, own, got,
            ] + [pl.BlockSpec(memory_space=pl.ANY)] * len(given),
            out_specs=pl.BlockSpec((pair, None, capacity, ff), lambda j, i, s: (i, 1 - s[0] if peer else s[0], 0, skip + j)),
        ),
        out_shape=jax.ShapeDtypeStruct((devices, 2, capacity, ff_dim), jnp.bfloat16),
        input_output_aliases={7: 0} if given else {},
        compiler_params=pltpu.CompilerParams(dimension_semantics=("arbitrary", "arbitrary"), vmem_limit_bytes=48 * 2**20),
        cost_estimate=pl.CostEstimate(flops=4 * rows * model_dim * size, bytes_accessed=2 * (rows * model_dim + 2 * model_dim * size + rows * size), transcendentals=rows * size),
        name="expert_up",
    )(ids, z, z, wg_own, wg_got, wu_own, wu_got, *given)


def down_kernel(ids_ref, mid_ref, *refs):
    out_ref = refs[-1]
    w = [r[0] if len(r.shape) == 3 else r[...] for r in refs[:-1]]
    w = w[0] if len(w) == 1 else jnp.concatenate(w, axis=1)
    out_ref[...] = jnp.dot(mid_ref[...], w, preferred_element_type=jnp.float32).astype(out_ref.dtype)


def expert_down(ids, mid, weights, specs, cols):
    rows, ff_dim = mid.shape
    rb = tile_of(rows, 512)
    return pl.pallas_call(
        down_kernel,
        grid_spec=pltpu.PrefetchScalarGridSpec(
            num_scalar_prefetch=1,
            grid=(rows // rb,),
            in_specs=[pl.BlockSpec((rb, ff_dim), lambda i, s: (i, 0))] + specs,
            out_specs=pl.BlockSpec((rb, cols), lambda i, s: (i, 0)),
        ),
        out_shape=jax.ShapeDtypeStruct((rows, cols), jnp.bfloat16),
        compiler_params=pltpu.CompilerParams(dimension_semantics=("arbitrary",), vmem_limit_bytes=48 * 2**20),
        cost_estimate=pl.CostEstimate(flops=2 * rows * cols * ff_dim, bytes_accessed=2 * (rows * cols + cols * ff_dim + rows * ff_dim), transcendentals=0),
    )(ids, mid, *weights)


def combine_kernel(hid_ref, scale_ref, *refs):
    out_ref = refs[-1]
    half = out_ref.shape[1] // 2
    sides = [hid_ref[:, :half].astype(jnp.float32), hid_ref[:, half:].astype(jnp.float32)]
    mixed = [None, None]
    for k in range(len(refs) // 2):
        early, late = refs[2 * k], refs[2 * k + 1]
        own = early[:, :half].astype(jnp.float32)
        other = jnp.concatenate([early[:, half:], late[...]], axis=1).astype(jnp.float32)
        gate = scale_ref[:, 2 * k:2 * k + 1]
        flip = scale_ref[:, 2 * k + 1:2 * k + 2] > 0
        for side, value in enumerate((jnp.where(flip, other, own), jnp.where(flip, own, other))):
            term = value * gate
            mixed[side] = term if mixed[side] is None else mixed[side] + term
    out_ref[:, :half] = (sides[0] + mixed[0]).astype(out_ref.dtype)
    out_ref[:, half:] = (sides[1] + mixed[1]).astype(out_ref.dtype)


def combine(hidden, scale, parts):
    rows, model_dim = hidden.shape
    rb = 256
    return pl.pallas_call(
        combine_kernel,
        grid=(rows // rb,),
        in_specs=[pl.BlockSpec((rb, a.shape[1]), lambda i: (i, 0)) for a in (hidden, scale, *parts)],
        out_specs=pl.BlockSpec((rb, model_dim), lambda i: (i, 0)),
        out_shape=jax.ShapeDtypeStruct((rows, model_dim), jnp.bfloat16),
        compiler_params=pltpu.CompilerParams(dimension_semantics=("arbitrary",), vmem_limit_bytes=48 * 2**20),
        cost_estimate=pl.CostEstimate(flops=8 * rows * model_dim, bytes_accessed=8 * rows * model_dim, transcendentals=0),
        name="combine",
    )(hidden, scale, *parts)


def solution(mesh):
    tok_spec = P(('rep', 'expert', 'data'), None, None)
    group_axes = ('data', 'expert')
    token_axes = ('expert', 'data')
    data_size, expert_size = mesh.shape['data'], mesh.shape['expert']
    num_experts = expert_size * data_size
    other_data = [(0, 1), (1, 0)]
    other_chip = [(e, e ^ 2) for e in range(expert_size)]
    other_core = [(e, e ^ 1) for e in range(expert_size)]

    def local_step(x_loc, idx_loc, gate_loc, attn_gain, qkv_part, out_part, moe_gain, gate_part, up_part, down_part):
        num_seqs, seq_len, model_dim = x_loc.shape
        num_heads, head_dim = out_part.shape[0], out_part.shape[1]
        tok_dev = num_seqs * seq_len
        top_k = idx_loc.shape[-1]
        capacity = capacity_of(tok_dev, top_k, num_experts)
        half, ff_dim = gate_part.shape[1:]
        mine = lax.axis_index('data')
        place = lax.axis_index('expert')

        ids = jnp.stack([mine.astype(jnp.int32)])
        theirs = 1 - mine

        def swap(value):
            return lax.ppermute(value, 'data', other_data)

        def cross(value):
            return lax.ppermute(value, 'expert', other_chip)

        def plan(flat_ids):
            slot_pos = slots_of(flat_ids, num_experts)
            kept = slot_pos < capacity
            here = kept & (flat_ids % data_size == mine)
            slot = jnp.where(here, flat_ids // data_size * capacity + slot_pos, expert_size * capacity)
            source = jnp.zeros((expert_size * capacity,), jnp.int32)
            source = source.at[slot].set(jnp.arange(tok_dev * top_k, dtype=jnp.int32) // top_k, mode='drop')
            return kept, slot_pos, source

        flat_ids = idx_loc.reshape(tok_dev * top_k)
        kept, slot_pos, source = plan(flat_ids)
        _, _, peer_source = plan(swap(flat_ids))

        def dispatch(normed, source):
            send = normed.at[source].get(mode='promise_in_bounds')
            return lax.all_to_all(send.reshape(expert_size, capacity, model_dim), 'expert', 0, 0, tiled=True).reshape(-1, model_dim)

        def spread(part, first):
            row = lax.dynamic_update_slice(jnp.zeros((data_size, expert_size) + part.shape, part.dtype), part[None, None], (mine, place, 0, 0))
            along, over, row, first = lax.optimization_barrier((swap(part), cross(part), row, first))
            whole = row
            for row, pieces in ((mine, [part, over]), (1 - mine, [along, cross(along)])):
                for chip, piece in enumerate(pieces):
                    there = place ^ (2 * chip)
                    if piece is not part:
                        whole = lax.dynamic_update_slice(whole, piece[None, None], (row, there, 0, 0))
                    whole = lax.dynamic_update_slice(whole, lax.ppermute(piece, 'expert', other_core)[None, None], (row, there ^ 1, 0, 0))
            return whole.reshape(-1, part.shape[1]), first

        ff = tile_of(ff_dim, 384)
        split = ff_dim // ff * 3 // 5 * ff
        sends = [lax.dynamic_slice(p, (theirs, 0, first), (1, half, size))[0] for first, size in ((0, split), (split, ff_dim - split)) for p in (gate_part, up_part)]
        normed_x = rms_scale(x_loc, attn_gain).reshape(tok_dev, model_dim)
        out_t = out_part.reshape(num_heads * head_dim, -1).T
        qkv_part, out_t = lax.optimization_barrier((qkv_part, out_t))
        qkv_flat = qkv_part.reshape(qkv_part.shape[0], -1)
        w_qkv, (normed_x, source) = spread(qkv_flat, (normed_x, source))
        got = [swap(part)[None] for part in sends]
        more = half - half // 2 // 256 * 256
        got_down = [swap(lax.dynamic_slice(down_part, (theirs, 0, first), (1, ff_dim, size))[0]) for first, size in ((0, more), (more, half - more))]

        qkv = jnp.dot(normed_x, w_qkv, preferred_element_type=jnp.float32).astype(jnp.bfloat16)
        w_out_t, qkv = spread(out_t, qkv)
        attended = attention_core(qkv, num_seqs, num_heads, head_dim)
        attn_proj = lax.dot_general(attended, w_out_t, (((1,), (1,)), ((), ())), preferred_element_type=jnp.float32)
        hidden = (x_loc.reshape(tok_dev, model_dim).astype(jnp.float32) + attn_proj).astype(jnp.bfloat16)

        normed = rms_scale(hidden, moe_gain)
        peer_normed = swap(normed)
        own_rows = dispatch(normed, source)
        peer_rows = dispatch(peer_normed, peer_source)
        mid = None
        for first, wg_got, wu_got in ((0, got[0], got[1]), (split, got[2], got[3])):
            for rows, peer in ((own_rows, False), (peer_rows, True)):
                mid = expert_up(ids, rows, gate_part, wg_got, up_part, wu_got, mid, first, ff, capacity, peer)

        mid = mid.reshape(num_experts * capacity, ff_dim)

        once = pl.Buffered(buffer_count=1)
        spec_own = pl.BlockSpec((1, ff_dim, half), lambda i, s: (s[0], 0, 0), pipeline_mode=once)
        spec_got = [pl.BlockSpec(part.shape, lambda i, s: (0, 0), pipeline_mode=once) for part in got_down]

        def back(cols):
            return lax.all_to_all(cols.reshape(num_experts, capacity, -1), token_axes, 0, 0, tiled=True).reshape(num_experts * capacity, -1)

        outs = expert_down(ids, mid, [down_part, got_down[0]], [spec_own, spec_got[0]], half + more)
        outs, last_down = lax.optimization_barrier((outs, got_down[1]))
        last_outs = expert_down(ids, mid, [last_down], [spec_got[1]], half - more)
        pieces = [back(outs), back(last_outs)]

        pick = jnp.where(kept, flat_ids * capacity + slot_pos, 0).reshape(tok_dev, top_k)
        scale = jnp.where(kept, gate_loc.reshape(tok_dev * top_k), 0.0)
        odd = (flat_ids % data_size).astype(jnp.float32)
        scale = jnp.stack([scale, odd], axis=1).reshape(tok_dev, 2 * top_k)
        parts = [p.at[pick[:, k]].get(mode='promise_in_bounds') for k in range(top_k) for p in pieces]
        return combine(hidden, scale, parts).reshape(num_seqs, seq_len, model_dim)

    in_specs = (tok_spec, tok_spec, tok_spec, P(None), P(group_axes, None, None), P(None, None, group_axes), P(None), P('expert', 'data', None), P('expert', 'data', None), P('expert', None, 'data'))

    return jax.shard_map(local_step, mesh=mesh, in_specs=in_specs, out_specs=tok_spec, check_vma=False)
```
